32 devices in a mesh: grp: 2 (over y), ka: 4 (over z), ga: 2 (over x), ba: 2 (over core).
Axes of the slice: x: 2, y: 2, z: 4, core: 2. Of those that a mesh axis runs over, the one named last changes fastest.
Arguments:
- coefficients: bfloat16 [2, 2, 16, 512, 9216], P(None, None, ('grp', 'ka'), 'ba', 'ga'), parts along dimension 2, may hold values from -1 to 1
- occupied: int32 [2, 16], P(None, ('grp', 'ka')), parts along dimension 1, may hold values from 64 to 512
- kweights: float32 [16], P(('grp', 'ka')), parts along dimension 0, may hold values from 0.5 to 2
- owner_map: int32 [1024], P('grp'), parts along dimension 0, may hold values from 0 to 7, as said below
- species: int32 [1024], P('grp'), parts along dimension 0, may hold values from 0 to 1
- positions: float32 [3, 1024], P(None, 'grp'), parts along dimension 1, may hold values from 0 to 100
- multipole: float32 [2, 9, 324], replicated, may hold values from -0.3125 to 0.3125
- widths: float32 [2], replicated, may hold values from 0.05 to 0.3
- potential: float32 [2, 442368], P(None, ('grp', 'ga')), parts along dimension 1, may hold values from -0.013671875 to 0.013671875
Outputs:
- density: float32 [2, 2, 1024, 324], P(None, None, ('grp', 'ka', 'ga', 'ba')), parts along dimension 2
- forces: float32 [3, 1024], P(None, ('grp', 'ka', 'ga', 'ba')), parts along dimension 1
The draws below stay inside these ranges and needn't reach their ends.
There are 2 independent parts, one for each index of `grp`. The reference program is written for one: setup_inputs(seed, part) draws one part's arguments, and reference() takes and returns one part's arrays. A program takes and returns all parts, laid end to end along the dimension named above; an argument that names none is the same for every part. Nothing has to cross between parts.
Inputs may be any that keep to these rules, and one draw needn't show every extreme that they name: `owner_map`: within each aligned block of 256 atoms every owner number is named by exactly 32 atoms.
All inputs are finite; a program needn't handle non-finite values.
Results may differ from the reference program's by a relative error of at most 0.0003.
Values sent between devices are 32-bit elements; how exact they have to be, the bound alone decides.
A program may use at most 192 MiB of HBM per device.

```python
import math
import jax
import jax.numpy as jnp
from jax import lax

NSPIN = 2
NPROJ = 18
ATOMS = 512
SPECIES = 2
NL = 9
GRID = 96
G_DEV = 110592
KPTS = 8
BANDS = 512
GTOT = 221184
ATOMS_BLK = 256
PER_OWN = 32
N_GA = 2
N_BA = 2


def draw_coefficients(key, part):
    keys = jax.random.split(key, 4)
    dims_all = (NSPIN, KPTS, BANDS, ATOMS, NPROJ)
    spread = (KPTS * BANDS) ** (-0.5)
    real_noise = jax.random.normal(keys[0], dims_all, jnp.float32)
    imag_noise = jax.random.normal(keys[1], dims_all, jnp.float32)
    mix_real = jax.random.normal(keys[2], (ATOMS, NPROJ, NPROJ), jnp.float32) / 6.0
    mix_imag = jax.random.normal(keys[3], (ATOMS, NPROJ, NPROJ), jnp.float32) / 6.0
    real_part = spread * (jnp.einsum('skbai,aij->skbaj', real_noise, mix_real) - jnp.einsum('skbai,aij->skbaj', imag_noise, mix_imag))
    imag_part = spread * (jnp.einsum('skbai,aij->skbaj', real_noise, mix_imag) + jnp.einsum('skbai,aij->skbaj', imag_noise, mix_real))
    stacked = jnp.stack([real_part, imag_part], axis=1).reshape(NSPIN, 2, KPTS, BANDS, ATOMS * NPROJ)
    return jnp.clip(stacked, -1.0, 1.0).astype(jnp.bfloat16)


def draw_owner_map(key, part):
    blocks = ATOMS // ATOMS_BLK

    def one_block(number):
        return jax.random.permutation(jax.random.fold_in(key, number), ATOMS_BLK)
    shuffled = jax.vmap(one_block)(jnp.arange(blocks, dtype=jnp.int32))
    return (shuffled // PER_OWN).reshape(ATOMS).astype(jnp.int32)


def place_ends(values, key, least, high):
    shape = values.shape
    index_at = [jax.random.randint(jax.random.fold_in(key, axis), (), 0, shape[axis]) for axis in range(len(shape))]
    values = values.at[tuple(index_at)].set(least)
    longest = shape.index(max(shape))
    index_at[longest] = (index_at[longest] + 1) % shape[longest]
    return values.at[tuple(index_at)].set(high)


def block_scale(stream_key, extent, cuts, smallest, high):
    gain, own = 1.0, jax.random.fold_in(stream_key, 6)
    for axis_at, parts in cuts:
        steps = jnp.exp(jax.random.uniform(jax.random.fold_in(own, axis_at), (parts,), jnp.float32, smallest / len(cuts), high / len(cuts)))
        gain = gain * jnp.repeat(steps, extent[axis_at] // parts).reshape([-1 if axis == axis_at else 1 for axis in range(len(extent))])
    return gain


def centred(rng, shape, width, reach, shards=(), kind=jnp.bfloat16):
    factor_of = block_scale(rng, shape, shards, -0.22, 0.18) if shards else 1.0
    array = jax.random.normal(rng, shape, jnp.float32) * width * factor_of
    return jnp.minimum(jnp.maximum(array, -reach), reach).astype(kind)


def setup_inputs(seed: int = 0, part: int = 0) -> dict:
    streams_of = jax.random.split(jax.random.key(seed), 10)
    part_splits = jax.random.split(jax.random.fold_in(streams_of[9], part), 10)
    return {
        "coefficients": draw_coefficients(jax.random.fold_in(jax.random.fold_in(streams_of[9], part), 71), part),
        "occupied": place_ends(jax.random.randint(part_splits[1], (NSPIN, KPTS), BANDS // 8, BANDS + 1), jax.random.fold_in(part_splits[1], 1), BANDS // 8, BANDS).astype(jnp.int32),
        "kweights": jnp.clip(jnp.exp(math.log(2.0) - 1.3862944 * jax.random.uniform(part_splits[2], (KPTS,), jnp.float32) ** block_scale(part_splits[2], (KPTS,), ((0, 4),), -0.2, 0.2)), 0.5, 2.0),
        "owner_map": draw_owner_map(jax.random.fold_in(jax.random.fold_in(streams_of[9], part), 71), part),
        "species": place_ends(jax.random.randint(part_splits[4], (ATOMS,), 0, SPECIES), jax.random.fold_in(part_splits[4], 1), 0, SPECIES - 1).astype(jnp.int32),
        "positions": jnp.clip(jax.random.uniform(part_splits[5], (3, ATOMS), jnp.float32, 0.0, 100.0), 0.0, 100.0),
        "multipole": centred(streams_of[6], (SPECIES, NL, NPROJ * NPROJ), (NPROJ * NPROJ) ** -0.5, 0.3125, (), jnp.float32),
        "widths": jnp.clip(jnp.exp(jax.random.uniform(streams_of[7], (SPECIES,), jnp.float32, math.log(0.05), math.log(0.3))), 0.05, 0.3),
        "potential": centred(part_splits[8], (2, GTOT), GTOT ** -0.5, 0.013671875, ((1, 2),), jnp.float32),
    }


grid_step = 0.0625
highest = lax.Precision.HIGHEST


def harmonics(start_index, length, widths):
    indices = start_index + jnp.arange(length, dtype=jnp.int32)
    planes = [indices % GRID, (indices // GRID) % GRID, indices // (GRID * GRID)]
    vectors = []
    for plane_index in planes:
        signed = jnp.where(plane_index >= GRID // 2, plane_index - GRID, plane_index)
        vectors.append(grid_step * signed.astype(jnp.float32))
    along_x, along_y, along_z = vectors
    square = along_x * along_x + along_y * along_y + along_z * along_z
    shapes = jnp.stack([jnp.ones_like(square), along_x, along_y, along_z, along_x * along_y, along_y * along_z, along_z * along_x, along_x * along_x - along_y * along_y, 3.0 * along_z * along_z - square])
    damping = jnp.exp(-widths[:, None] * square[None, :])
    form_table = (damping[:, None, :] * shapes[None, :, :]).reshape(SPECIES * NL, length)
    return form_table, jnp.stack(vectors, axis=1)


def force_block(moments, places, form_table, vectors, pot_piece):
    smooth = jnp.dot(moments, form_table, precision=highest)
    phases = jnp.dot(places, vectors.T, precision=highest)
    wave_term = pot_piece[0][None, :] * jnp.sin(phases) + pot_piece[1][None, :] * jnp.cos(phases)
    return jnp.dot(smooth * wave_term, vectors, precision=highest)


def reference(coefficients, occupied, kweights, owner_map, species, positions, multipole, widths, potential):
    band_index = jnp.arange(BANDS, dtype=jnp.int32)
    band_masks = (band_index[None, None, :] < occupied[:, :, None]).astype(jnp.float32)

    def kpoint(running, inputs):
        kpoint_slab, band_mask, weight = inputs
        values = kpoint_slab.astype(jnp.float32).reshape(NSPIN, 2, BANDS, ATOMS, NPROJ)
        masked = values * band_mask[:, None, :, None, None]
        real_part = jnp.einsum("scnai,scnaj->saij", values, masked)
        cross_term = jnp.einsum("snai,snaj->saij", values[:, 0], masked[:, 1])
        imag_part = cross_term - jnp.swapaxes(cross_term, 2, 3)
        return running + weight * jnp.stack([real_part, imag_part], axis=1), None

    initial = jnp.zeros((NSPIN, 2, ATOMS, NPROJ, NPROJ), jnp.float32)
    density_all, unused = lax.scan(kpoint, initial, (jnp.moveaxis(coefficients, 2, 0), jnp.moveaxis(band_masks, 1, 0), kweights))
    density_all = density_all.reshape(NSPIN, 2, ATOMS, NPROJ * NPROJ)
    atom_index = jnp.arange(ATOMS, dtype=jnp.int32)
    sort_key = ((owner_map // N_BA) * N_GA + atom_index // ATOMS_BLK) * N_BA + owner_map % N_BA
    ordering = jnp.argsort(sort_key, stable=True).astype(jnp.int32)
    density = jnp.take(density_all, ordering, axis=2)
    real_total = jnp.sum(density_all[:, 0], axis=0)
    selector = (species[:, None] == jnp.arange(SPECIES, dtype=jnp.int32)[None, :]).astype(jnp.float32)
    moments = jnp.dot(real_total, multipole.reshape(SPECIES * NL, NPROJ * NPROJ).T, precision=highest) * jnp.repeat(selector, NL, axis=1)
    block_size = G_DEV // 8
    places = positions.T

    def gblock(running, number):
        start_index = number * block_size
        form_table, vectors = harmonics(start_index, block_size, widths)
        pot_piece = lax.dynamic_slice_in_dim(potential, start_index, block_size, 1)
        return running + force_block(moments, places, form_table, vectors, pot_piece), None

    force_all, unused = lax.scan(gblock, jnp.zeros((ATOMS, 3), jnp.float32), jnp.arange(GTOT // block_size, dtype=jnp.int32))
    forces = jnp.take(force_all, ordering, axis=0).T
    return density, forces
```

```python
import functools
import math

import jax
import jax.numpy as jnp
import numpy as np
from jax import lax
from jax.experimental import pallas as pl
from jax.experimental.pallas import tpu as pltpu
from jax.sharding import PartitionSpec as P

NPROJ = 18
SPECIES = 2
NL = 9
GRID = 96
LANES = 128
SUB = 8
ENTRIES = NPROJ * NPROJ
PAD = -(-ENTRIES // LANES) * LANES
WIN = SUB * NPROJ
SLOTS = 2
HALF = LANES // 2
CHUNK = 3

grid_step = 0.0625
highest = lax.Precision.HIGHEST


def group_width():
    return NPROJ * LANES // math.gcd(NPROJ, LANES)


@functools.lru_cache(None)
def fold_table():
    q = np.zeros((PAD, PAD), np.float32)
    for i in range(NPROJ):
        for j in range(i):
            q[i * NPROJ + j, i * NPROJ + j] += 1.0
            q[j * NPROJ + i, i * NPROJ + j] -= 1.0
    return q


@functools.lru_cache(None)
def open_table():
    u = np.zeros((PAD, 2 * PAD), np.float32)
    for i in range(NPROJ):
        for j in range(NPROJ):
            u[min(i, j) * NPROJ + max(i, j), i * NPROJ + j] = 1.0
            if i > j:
                u[i * NPROJ + j, PAD + i * NPROJ + j] = 1.0
            elif i < j:
                u[j * NPROJ + i, PAD + i * NPROJ + j] = -1.0
    return u


POWERS = [(i, j, k) for i in range(4) for j in range(4 - i) for k in range(4 - i - j)]
SHAPES = [
    {(0, 0, 0): 1.0},
    {(1, 0, 0): 1.0},
    {(0, 1, 0): 1.0},
    {(0, 0, 1): 1.0},
    {(1, 1, 0): 1.0},
    {(0, 1, 1): 1.0},
    {(1, 0, 1): 1.0},
    {(2, 0, 0): 1.0, (0, 2, 0): -1.0},
    {(0, 0, 2): 2.0, (2, 0, 0): -1.0, (0, 2, 0): -1.0},
]
KIND_ROW = len(POWERS)
ROWS = -(-(KIND_ROW + 1) // SUB) * SUB


def split(value):
    high = value.astype(jnp.bfloat16)
    return high, (value - high.astype(jnp.float32)).astype(jnp.bfloat16)


def mdot(a, b):
    return jnp.dot(a, b, preferred_element_type=jnp.float32)


def flags(value):
    return value.astype(jnp.float32).astype(jnp.bfloat16)


def before(count):
    row = lax.broadcasted_iota(jnp.int32, (count, count), 0)
    col = lax.broadcasted_iota(jnp.int32, (count, count), 1)
    return flags(row < col)


def gram_kernel(occ_ref, weight_ref, x_hbm, owner_ref, fold_ref, out_ref, x_ref, xa_ref, xb_ref, sc_ref, t_ref, sems):
    spins, groups, _, kcount, bcount, width = x_ref.shape
    atoms = t_ref.shape[2]
    per = width // NPROJ
    total = spins * groups

    def fetch(n):
        s, g = n // groups, n % groups
        return pltpu.make_async_copy(
            x_hbm.at[s, :, :, :, pl.ds(pl.multiple_of(g*width, width), width)], x_ref.at[s, g], sems.at[s, g])

    for n in range(total):
        fetch(n).start()
    band = lax.broadcasted_iota(jnp.int32, (LANES, bcount), 1) + lax.axis_index("ba") * bcount
    lane = lax.broadcasted_iota(jnp.int32, (SUB, LANES), 1)
    row = lax.broadcasted_iota(jnp.int32, (SUB, LANES), 0)
    shifts = [NPROJ*row + (at*LANES + lane) % NPROJ for at in range(PAD//LANES)]
    past = lax.broadcasted_iota(jnp.int32, (WIN, LANES), 1) - lax.broadcasted_iota(
        jnp.int32, (WIN, LANES), 0) // NPROJ * NPROJ

    def turn(n, xt_ref, t):
        s, g = n // groups, n % groups
        cols = slice(t*LANES, (t+1)*LANES)
        for k in range(kcount):
            mask = (band < occ_ref[s, k]).astype(jnp.float32).astype(jnp.bfloat16)
            for c in range(2):
                v = x_ref[s, g, c, k, :, cols].T * mask
                at = t*LANES
                while at < (t+1)*LANES:
                    w = at // WIN
                    end = min((w+1)*WIN, (t+1)*LANES)
                    xt_ref[k, w, (1-c)*WIN + at - w*WIN:(1-c)*WIN + end - w*WIN, :] = v[at - t*LANES:end - t*LANES]
                    at = end

    def window(n, xt_ref, w):
        s, g = n // groups, n % groups
        base = (w*WIN)//LANES*LANES
        o = w*WIN - base
        win = slice(base, base + 2*LANES)
        take = past < o + NPROJ - LANES
        re = im = None
        for k in range(kcount):
            both = mdot(xt_ref[k, w], x_ref[s, g, 1, k, :, win])
            r = mdot(xt_ref[k, w, WIN:], x_ref[s, g, 0, k, :, win]) + both[:WIN]
            m = both[WIN:]
            weight = weight_ref[k]
            r = jnp.where(take, r[:, LANES:], r[:, :LANES]) * weight
            m = jnp.where(take, m[:, LANES:], m[:, :LANES]) * weight
            re = r if re is None else re + r
            im = m if im is None else im + m
        sc_ref[w % SLOTS, 0] = re
        sc_ref[w % SLOTS, 1] = im

    def unfold(n, w):
        s, g = n // groups, n % groups
        o = w*WIN % LANES
        lifts = [(o + shift) & (LANES - 1) for shift in shifts]
        for c in range(2):
            tiles = [None]*(PAD//LANES)
            for i in range(NPROJ):
                piece = sc_ref[w % SLOTS, c, pl.ds(i, SUB, stride=NPROJ), :]
                for at in range(i*NPROJ // LANES, (i*NPROJ + NPROJ - 1) // LANES + 1):
                    part = jnp.take_along_axis(piece, lifts[at], axis=1, mode="promise_in_bounds")
                    tiles[at] = part if tiles[at] is None else jnp.where(lane >= i*NPROJ - at*LANES, part, tiles[at])
            for at, v in enumerate(tiles):
                here = pl.multiple_of(g*per + w*SUB, SUB)
                t_ref[s, c, pl.ds(here, SUB), at*LANES:(at+1)*LANES] = v

    fetch(0).wait()
    for t in range(width // LANES):
        turn(0, xa_ref, t)

    def step(n, here, there):
        after = jnp.minimum(n + 1, total - 1)
        @pl.when(n + 1 < total)
        def _():
            fetch(n + 1).wait()
        for w in range(width // WIN):
            window(n, here, w)
            turn(after, there, w)
            if w == 0:
                turn(after, there, width // LANES - 1)
            unfold(n, w)

    @pl.loop(0, total // 2)
    def _(pair):
        step(2*pair, xa_ref, xb_ref)
        step(2*pair + 1, xb_ref, xa_ref)

    e = lax.broadcasted_iota(jnp.int32, (atoms, PAD), 1)
    keep = (e // NPROJ <= e % NPROJ) & (e < ENTRIES)
    q = fold_ref[...]
    owners = lax.axis_size("ka") * lax.axis_size("ba")
    owner = owner_ref[:, :atoms]
    for block in range(1, owner_ref.shape[1] // atoms):
        piece = owner_ref[:, block * atoms:(block + 1) * atoms]
        owner = jnp.where(lax.axis_index("ga") == block, piece, owner)
    member = lax.broadcasted_iota(jnp.int32, (max(owners, 2 * SUB), atoms), 0) == owner
    count = mdot(flags(member), before(atoms))
    rank = jnp.sum(jnp.where(member, count, 0.0), axis=0, keepdims=True)
    spot = owner.astype(jnp.float32) * (atoms // owners) + rank
    place = lax.broadcasted_iota(jnp.int32, (atoms, atoms), 0).astype(jnp.float32)
    route = flags(place == spot)
    for s in range(spins):
        hi, lo = split(jnp.where(e < ENTRIES, t_ref[s, 1], 0.0))
        h = jnp.where(keep, t_ref[s, 0], 0.0) + (mdot(hi, q) + mdot(lo, q))
        hi, lo = split(h)
        out_ref[s] = mdot(route, hi) + mdot(route, lo)


def gram(coefficients, occupied, kweights, owner_map):
    spins, parts, kcount, bcount, columns = coefficients.shape
    width = group_width()
    groups = columns // width
    atoms = columns // NPROJ
    vmem = pl.BlockSpec(memory_space=pltpu.VMEM)
    smem = pl.BlockSpec(memory_space=pltpu.SMEM)
    return pl.pallas_call(
        gram_kernel,
        out_shape=jax.ShapeDtypeStruct((spins, atoms, PAD), jnp.float32),
        in_specs=[smem, smem, pl.BlockSpec(memory_space=pl.ANY), vmem, vmem],
        out_specs=vmem,
        scratch_shapes=[
            pltpu.VMEM((spins, groups, parts, kcount, bcount, width), jnp.bfloat16),
            *[pltpu.VMEM((kcount, width // WIN, 2 * WIN, bcount), jnp.bfloat16)] * 2,
            pltpu.VMEM((SLOTS, 2, WIN, LANES), jnp.float32),
            pltpu.VMEM((spins, 2, atoms, PAD), jnp.float32),
            pltpu.SemaphoreType.DMA((spins, groups)),
        ],
        compiler_params=pltpu.CompilerParams(vmem_limit_bytes=48 * 2**20),
    )(occupied, kweights, coefficients, owner_map, jnp.asarray(fold_table(), jnp.bfloat16))


def sincos(angle):
    turns = jnp.floor(angle * (2.0 / math.pi) + 0.5)
    rest = ((angle - turns * 1.5703125) - turns * 4.837512969970703125e-4) - turns * 7.54978995489188216e-8
    z = rest * rest
    sine = ((-1.9515295891e-4 * z + 8.3321608736e-3) * z - 1.6666654611e-1) * z * rest + rest
    cosine = (
        (2.443315711809948e-5 * z - 1.388731625493765e-3) * z + 4.166664568298827e-2
    ) * z * z - 0.5 * z + 1.0
    quarter = turns.astype(jnp.int32) & 3
    odd = (quarter & 1) == 1
    s = jnp.where(odd, cosine, sine)
    c = jnp.where(odd, sine, cosine)
    return jnp.where(quarter >= 2, -s, s), jnp.where((quarter == 1) | (quarter == 2), -c, c)


def signed_steps(index):
    return grid_step * jnp.where(index >= GRID // 2, index - GRID, index).astype(jnp.float32)


def finish_kernel(
    width_ref, rows_ref, owner_ref, kind_ref, place_ref, grid_ref, total_ref, terms_ref,
    first, held, second, sent, third, left_ref, cosy_ref, siny_ref, cosz_ref, sinz_ref,
    send1, recv1, send2, recv2, send3, recv3,
):
    mesh_id = pl.DeviceIdType.MESH
    ka, ba, ga = (lax.axis_size(name) for name in ("ka", "ba", "ga"))
    k, b, g = (lax.axis_index(name) for name in ("ka", "ba", "ga"))
    per = rows_ref.shape[3]
    blocks = ga
    atoms = owner_ref.shape[1] // blocks
    barrier = pltpu.get_barrier_semaphore()
    for name, me, size in (("ka", k, ka), ("ba", b, ba), ("ga", g, ga)):
        for step in range(1, size):
            pl.semaphore_signal(
                barrier, inc=1, device_id={name: lax.rem(me + step, size)}, device_id_type=mesh_id
            )
    pl.semaphore_wait(barrier, ka + ba + ga - 3)

    copies1, copies2, copies3 = {}, {}, {}
    turns = [t // 2 + 1 if t % 2 == 0 else ka - 1 - t // 2 for t in range(ka - 1)][::-1] + [0]
    for turn in turns:
        to = lax.rem(k + turn, ka)
        for step in range(1, ba):
            peer = lax.rem(b + step, ba)
            copy = pltpu.make_async_remote_copy(
                src_ref=rows_ref.at[:, to, peer],
                dst_ref=first.at[step - 1, turn],
                send_sem=send1.at[step - 1, turn],
                recv_sem=recv1.at[step - 1, turn],
                device_id={"ba": peer},
                device_id_type=mesh_id,
            )
            copy.start()
            copies1[turn, step] = copy

    columns = []
    for block in range(blocks):
        span = slice(block * atoms, (block + 1) * atoms)
        mine = owner_ref[:, span] == k * ba + b
        rank = mdot(jnp.broadcast_to(flags(mine), (2 * SUB, atoms)), before(atoms))[:1]
        spot = lax.broadcasted_iota(jnp.int32, (per, atoms), 0).astype(jnp.float32)
        chosen = mine & (rank == spot)
        columns.append([
            jnp.sum(jnp.where(chosen, value, 0.0), axis=1, keepdims=True)
            for value in (
                place_ref[0:1, span], place_ref[1:2, span], place_ref[2:3, span],
                kind_ref[:, span].astype(jnp.float32),
            )
        ])
    lane = lax.broadcasted_iota(jnp.int32, (HALF, LANES), 1)
    table = jnp.zeros((HALF, LANES), jnp.float32)
    spare = HALF - blocks * per
    for at in range(4):
        pieces = [columns[block][at] for block in range(blocks)]
        if spare:
            pieces.append(jnp.zeros((spare, 1), jnp.float32))
        table = jnp.where(lane == at, jnp.concatenate(pieces, axis=0), table)
    flat = jnp.concatenate([table, table], axis=0).T
    kinds = flat[3:4]
    spread = jnp.where(kinds == 0.0, width_ref[0], width_ref[1])

    steps = signed_steps(lax.broadcasted_iota(jnp.int32, (GRID, LANES), 0))
    damp = jnp.exp(-spread * (steps * steps))
    sine, cosine = sincos(flat[0:1] * steps)
    sine, cosine = sine * damp, cosine * damp
    power = jnp.where(lax.broadcasted_iota(jnp.int32, (GRID, LANES), 1) < HALF, 1.0, steps)
    for pair in range(2):
        c, s = power * cosine, power * sine
        for at, value in enumerate((
            jnp.concatenate([c, s], axis=0), jnp.concatenate([s, -c], axis=0)
        )):
            high, low = split(value)
            cols = slice((2 * at + pair) * LANES, (2 * at + pair + 1) * LANES)
            left_ref[0, :, cols] = high
            left_ref[1, :, cols] = low
        power = power * (steps * steps)
    sine, cosine = sincos(flat[1:2] * steps)
    siny_ref[...] = sine * damp
    cosy_ref[...] = cosine * damp
    planes = grid_ref.shape[0] // GRID
    depth = sinz_ref.shape[0]
    deep = signed_steps(g * planes + lax.broadcasted_iota(jnp.int32, (depth, LANES), 0))
    sine, cosine = sincos(flat[2:3] * deep)
    damp = jnp.exp(-spread * (deep * deep))
    sinz_ref[...] = sine * damp
    cosz_ref[...] = cosine * damp

    for turn in turns[:-1]:
        to = lax.rem(k + turn, ka)
        value = rows_ref[:, to, b]
        for step in range(1, ba):
            copies1[turn, step].wait_recv()
            value = value + first[step - 1, turn]
        held[turn - 1] = value
        copy = pltpu.make_async_remote_copy(
            src_ref=held.at[turn - 1],
            dst_ref=second.at[turn - 1],
            send_sem=send2.at[turn - 1],
            recv_sem=recv2.at[turn - 1],
            device_id={"ka": to},
            device_id_type=mesh_id,
        )
        copy.start()
        copies2[turn] = copy

    line = steps[:, :1]

    def plane(z, carry, along):
        sums = list(carry)
        cz, sz = cosz_ref[pl.ds(z, 1), :], sinz_ref[pl.ds(z, 1), :]
        cy, sy = cosy_ref[...], siny_ref[...]
        cosine = cz * cy - sz * sy
        sine = sz * cy + cz * sy
        index = g * planes + z
        height = grid_step * jnp.where(index >= GRID // 2, index - GRID, index).astype(jnp.float32)
        at = 0
        for pair in range(2):
            wave = along[:, pair * LANES:(pair + 1) * LANES] * cosine
            wave = wave - along[:, (2 + pair) * LANES:(3 + pair) * LANES] * sine
            for j in range(4 - 2 * pair):
                part = jnp.sum(wave.reshape(GRID // SUB, SUB, LANES), axis=0)
                for _ in range(4 - 2 * pair - j):
                    sums[at] = sums[at] + part
                    part = part * height
                    at += 1
                wave = wave * line
        return tuple(sums)

    def body(chunk, carry):
        start = pl.multiple_of(chunk * CHUNK * GRID, GRID)
        high, low = split(grid_ref[pl.ds(start, CHUNK * GRID), :])
        along = mdot(high, left_ref[0]) + mdot(low, left_ref[0]) + mdot(high, left_ref[1])
        for turn in range(CHUNK):
            carry = plane(chunk * CHUNK + turn, carry, along[turn * GRID:(turn + 1) * GRID])
        return carry

    zero = jnp.zeros((SUB, LANES), jnp.float32)
    sums = lax.fori_loop(0, planes // CHUNK, body, (zero,) * 13)
    rows = {}
    at = 0
    for pair in range(2):
        for j in range(4 - 2 * pair):
            for l in range(4 - 2 * pair - j):
                value = jnp.sum(sums[at], axis=0, keepdims=True)
                at += 1
                rows[2 * pair, j, l] = value
                if 2 * pair + 1 + j + l <= 3:
                    rows[2 * pair + 1, j, l] = pltpu.roll(value, HALF, 1)
    pieces = [rows[power] for power in POWERS]
    mono = jnp.concatenate(pieces + [jnp.zeros((ROWS - len(pieces), LANES), jnp.float32)], axis=0)
    sent[...] = mono
    for step in range(1, ga):
        peer = lax.rem(g + step, ga)
        copy = pltpu.make_async_remote_copy(
            src_ref=sent,
            dst_ref=third.at[step - 1],
            send_sem=send3.at[step - 1],
            recv_sem=recv3.at[step - 1],
            device_id={"ga": peer},
            device_id_type=mesh_id,
        )
        copy.start()
        copies3[step] = copy

    value = rows_ref[:, k, b]
    for step in range(1, ba):
        copies1[0, step].wait_recv()
        value = value + first[step - 1, 0]
    for turn in turns[:-1][::-1]:
        copies2[turn].wait_recv()
        value = value + second[turn - 1]
    total_ref[...] = value
    for step in range(1, ga):
        copies3[step].wait_recv()
        mono = mono + third[step - 1]
    row = lax.broadcasted_iota(jnp.int32, (ROWS, LANES), 0)
    mono = jnp.where(row == KIND_ROW, kinds, mono)
    mine = mono
    for block in range(1, blocks):
        mine = jnp.where(g == block, pltpu.roll(mono, LANES - block * per, 1), mine)
    terms_ref[...] = mine
    for copy in [*copies1.values(), *copies2.values(), *copies3.values()]:
        copy.wait_send()


def finish(rows, owner_map, species, positions, widths, grid):
    spins, ka, ba, per, pad = rows.shape
    ga = lax.axis_size("ga")
    planes = grid.shape[0] // GRID
    chunk = (spins, per, pad)
    vmem = pl.BlockSpec(memory_space=pltpu.VMEM)
    smem = pl.BlockSpec(memory_space=pltpu.SMEM)
    return pl.pallas_call(
        finish_kernel,
        out_shape=(
            jax.ShapeDtypeStruct(chunk, jnp.float32),
            jax.ShapeDtypeStruct((ROWS, LANES), jnp.float32),
        ),
        in_specs=[smem] + [vmem] * 5,
        out_specs=(vmem, vmem),
        scratch_shapes=[
            pltpu.VMEM((ba - 1, ka, *chunk), jnp.float32),
            pltpu.VMEM((ka - 1, *chunk), jnp.float32),
            pltpu.VMEM((ka - 1, *chunk), jnp.float32),
            pltpu.VMEM((ROWS, LANES), jnp.float32),
            pltpu.VMEM((ga - 1, ROWS, LANES), jnp.float32),
            pltpu.VMEM((2, 2 * GRID, 4 * LANES), jnp.bfloat16),
            pltpu.VMEM((GRID, LANES), jnp.float32),
            pltpu.VMEM((GRID, LANES), jnp.float32),
            pltpu.VMEM((-(-planes // SUB) * SUB, LANES), jnp.float32),
            pltpu.VMEM((-(-planes // SUB) * SUB, LANES), jnp.float32),
            pltpu.SemaphoreType.DMA((ba - 1, ka)),
            pltpu.SemaphoreType.DMA((ba - 1, ka)),
            pltpu.SemaphoreType.DMA((ka - 1,)),
            pltpu.SemaphoreType.DMA((ka - 1,)),
            pltpu.SemaphoreType.DMA((ga - 1,)),
            pltpu.SemaphoreType.DMA((ga - 1,)),
        ],
        compiler_params=pltpu.CompilerParams(collective_id=0, has_side_effects=True),
    )(widths, rows, owner_map, species, positions, grid)


def tail_kernel(total_ref, terms_ref, multipole_ref, open_ref, density_ref, force_ref):
    spins, parts, per, entries = density_ref.shape
    high, low = split(total_ref[...])
    whole = mdot(high, open_ref[...]) + mdot(low, open_ref[...])
    real = None
    for s in range(spins):
        rows = slice(s * per, (s + 1) * per)
        density_ref[s, 0] = whole[rows, :entries]
        density_ref[s, 1] = whole[rows, PAD:PAD + entries]
        real = whole[rows, :entries] if real is None else real + whole[rows, :entries]
    moments = lax.dot_general(
        multipole_ref[...], real, (((1,), (1,)), ((), ())), precision=highest,
        preferred_element_type=jnp.float32,
    )
    kinds = terms_ref[KIND_ROW:KIND_ROW + 1, :per]
    moments = jnp.where(kinds == 0.0, moments[:NL], moments[NL:])
    index = {power: at for at, power in enumerate(POWERS)}
    for c in range(3):
        force = None
        for l, shape in enumerate(SHAPES):
            term = None
            for power, factor in shape.items():
                at = index[tuple(p + (axis == c) for axis, p in enumerate(power))]
                part = terms_ref[at:at + 1, :per] * factor
                term = part if term is None else term + part
            term = term * moments[l:l + 1]
            force = term if force is None else force + term
        force_ref[c:c + 1, :] = force


def tail(total, terms, multipole):
    spins, per, pad = total.shape
    return pl.pallas_call(
        tail_kernel,
        out_shape=(
            jax.ShapeDtypeStruct((spins, 2, per, ENTRIES), jnp.float32),
            jax.ShapeDtypeStruct((3, per), jnp.float32),
        ),
    )(
        total.reshape(spins * per, pad), terms, multipole.reshape(SPECIES * NL, ENTRIES),
        jnp.asarray(open_table(), jnp.bfloat16),
    )


def shards(
    coefficients, occupied, kweights, owner_map, species, positions, multipole, widths, potential
):
    spins = coefficients.shape[0]
    ka, ba = lax.axis_size("ka"), lax.axis_size("ba")
    owner_map = owner_map.reshape(1, -1)
    rows = gram(coefficients, occupied, kweights, owner_map)
    rows = rows.reshape(spins, ka, ba, -1, PAD)
    grid = potential.reshape(2, -1, GRID)
    grid = jnp.concatenate([grid[1], grid[0]], axis=1)
    total, terms = finish(rows, owner_map, species.reshape(1, -1), positions, widths, grid)
    return tail(total, terms, multipole)


def solution(mesh):
    placed = (
        P(None, None, ("grp", "ka"), "ba", "ga"),
        P(None, ("grp", "ka")),
        P(("grp", "ka")),
        P("grp"),
        P("grp"),
        P(None, "grp"),
        P(),
        P(),
        P(None, ("grp", "ga")),
    )
    return jax.shard_map(
        shards,
        mesh=mesh,
        in_specs=placed,
        out_specs=(
            P(None, None, ("grp", "ka", "ga", "ba"), None),
            P(None, ("grp", "ka", "ga", "ba")),
        ),
        check_vma=False,
    )
```

```python
import functools
import math

import jax
import jax.numpy as jnp
import numpy as np
from jax import lax
from jax.experimental import pallas as pl
from jax.experimental.pallas import tpu as pltpu
from jax.sharding import PartitionSpec as P

NPROJ = 18
SPECIES = 2
NL = 9
GRID = 96
LANES = 128
SUB = 8
ENTRIES = NPROJ * NPROJ
PAD = -(-ENTRIES // LANES) * LANES
WIN = SUB * NPROJ
SLOTS = 2
HALF = LANES // 2
CHUNK = 3
FOLD = 4

grid_step = 0.0625
highest = lax.Precision.HIGHEST


def group_width():
    return NPROJ * LANES // math.gcd(NPROJ, LANES)


@functools.lru_cache(None)
def fold_table():
    q = np.zeros((PAD, PAD), np.float32)
    for i in range(NPROJ):
        for j in range(i):
            q[i * NPROJ + j, i * NPROJ + j] += 1.0
            q[j * NPROJ + i, i * NPROJ + j] -= 1.0
    return q


@functools.lru_cache(None)
def open_table():
    u = np.zeros((PAD, 2 * PAD), np.float32)
    for i in range(NPROJ):
        for j in range(NPROJ):
            u[min(i, j) * NPROJ + max(i, j), i * NPROJ + j] = 1.0
            if i > j:
                u[i * NPROJ + j, PAD + i * NPROJ + j] = 1.0
            elif i < j:
                u[j * NPROJ + i, PAD + i * NPROJ + j] = -1.0
    return u


POWERS = [(i, j, k) for i in range(4) for j in range(4 - i) for k in range(4 - i - j)]
SHAPES = [
    {(0, 0, 0): 1.0},
    {(1, 0, 0): 1.0},
    {(0, 1, 0): 1.0},
    {(0, 0, 1): 1.0},
    {(1, 1, 0): 1.0},
    {(0, 1, 1): 1.0},
    {(1, 0, 1): 1.0},
    {(2, 0, 0): 1.0, (0, 2, 0): -1.0},
    {(0, 0, 2): 2.0, (2, 0, 0): -1.0, (0, 2, 0): -1.0},
]
KIND_ROW = len(POWERS)
ROWS = -(-(KIND_ROW + 1) // SUB) * SUB


def split(value):
    high = value.astype(jnp.bfloat16)
    return high, (value - high.astype(jnp.float32)).astype(jnp.bfloat16)


def mdot(a, b):
    return jnp.dot(a, b, preferred_element_type=jnp.float32)


def flags(value):
    return value.astype(jnp.float32).astype(jnp.bfloat16)


def before(count):
    row = lax.broadcasted_iota(jnp.int32, (count, count), 0)
    col = lax.broadcasted_iota(jnp.int32, (count, count), 1)
    return flags(row < col)


def sincos(angle):
    turns = jnp.floor(angle * (2.0 / math.pi) + 0.5)
    rest = ((angle - turns * 1.5703125) - turns * 4.837512969970703125e-4) - turns * 7.54978995489188216e-8
    z = rest * rest
    sine = ((-1.9515295891e-4 * z + 8.3321608736e-3) * z - 1.6666654611e-1) * z * rest + rest
    cosine = (
        (2.443315711809948e-5 * z - 1.388731625493765e-3) * z + 4.166664568298827e-2
    ) * z * z - 0.5 * z + 1.0
    quarter = turns.astype(jnp.int32) & 3
    odd = (quarter & 1) == 1
    s = jnp.where(odd, cosine, sine)
    c = jnp.where(odd, sine, cosine)
    return jnp.where(quarter >= 2, -s, s), jnp.where((quarter == 1) | (quarter == 2), -c, c)


def signed_steps(index):
    return grid_step * jnp.where(index >= GRID // 2, index - GRID, index).astype(jnp.float32)


def main_kernel(
    occ_ref, weight_ref, width_ref, x_hbm, wave_hbm, fold_hbm, open_hbm, owner_ref, kind_ref,
    place_ref, multipole_ref, density_ref, force_ref,
    x_ref, xa_ref, xb_ref, sc_ref, t_ref, route_ref, rows_ref, first, held, second, sent, third,
    wave_ref, fold_ref, open_ref, left_ref, cosy_ref, siny_ref, cosz_ref, sinz_ref,
    sems, loads, send1, recv1, send2, recv2, send3, recv3,
):
    mesh_id = pl.DeviceIdType.MESH
    ka, ba, ga = (lax.axis_size(name) for name in ("ka", "ba", "ga"))
    k, b, g = (lax.axis_index(name) for name in ("ka", "ba", "ga"))
    spins, groups, _, kcount, bcount, width = x_ref.shape
    atoms = t_ref.shape[1]
    per = rows_ref.shape[3]
    blocks = ga
    owners = ka * ba
    group_atoms = width // NPROJ
    total = spins * groups

    def fetch(n):
        s, group = n // groups, n % groups
        cols = pl.ds(pl.multiple_of(group * width, width), width)
        return pltpu.make_async_copy(
            x_hbm.at[s, :, :, :, cols], x_ref.at[s, group], sems.at[s, group]
        )

    others = [
        pltpu.make_async_copy(source, target, loads.at[at])
        for at, (source, target) in enumerate((
            (fold_hbm, fold_ref), (wave_hbm, wave_ref), (open_hbm, open_ref)
        ))
    ]
    fetch(0).start()
    for n in range(1, total):
        fetch(n).start()
        if n == 1:
            for copy in others:
                copy.start()
    barrier = pltpu.get_barrier_semaphore()
    for name, me, size in (("ka", k, ka), ("ba", b, ba), ("ga", g, ga)):
        for step in range(1, size):
            pl.semaphore_signal(
                barrier, inc=1, device_id={name: lax.rem(me + step, size)}, device_id_type=mesh_id
            )

    owner = owner_ref[:, :atoms]
    for block in range(1, blocks):
        piece = owner_ref[:, block * atoms:(block + 1) * atoms]
        owner = jnp.where(g == block, piece, owner)
    lower = before(atoms)
    member = lax.broadcasted_iota(jnp.int32, (max(owners, 2 * SUB), atoms), 0) == owner
    count = mdot(flags(member), lower)
    rank = jnp.sum(jnp.where(member, count, 0.0), axis=0, keepdims=True)
    spot = owner.astype(jnp.float32) * per + rank
    place = lax.broadcasted_iota(jnp.int32, (atoms, atoms), 0).astype(jnp.float32)
    route_ref[...] = flags(place == spot)

    columns = []
    for block in range(blocks):
        span = slice(block * atoms, (block + 1) * atoms)
        mine = owner_ref[:, span] == k * ba + b
        rank = mdot(jnp.broadcast_to(flags(mine), (2 * SUB, atoms)), lower)[:1]
        spot = lax.broadcasted_iota(jnp.int32, (per, atoms), 0).astype(jnp.float32)
        chosen = mine & (rank == spot)
        columns.append([
            jnp.sum(jnp.where(chosen, value, 0.0), axis=1, keepdims=True)
            for value in (
                place_ref[0:1, span], place_ref[1:2, span], place_ref[2:3, span],
                kind_ref[:, span].astype(jnp.float32),
            )
        ])
    index = lax.broadcasted_iota(jnp.int32, (HALF, LANES), 1)
    table = jnp.zeros((HALF, LANES), jnp.float32)
    spare = HALF - blocks * per
    for at in range(4):
        pieces = [columns[block][at] for block in range(blocks)]
        if spare:
            pieces.append(jnp.zeros((spare, 1), jnp.float32))
        table = jnp.where(index == at, jnp.concatenate(pieces, axis=0), table)
    flat = jnp.concatenate([table, table], axis=0).T
    kinds = flat[3:4]
    spread = jnp.where(kinds == 0.0, width_ref[0], width_ref[1])

    steps = signed_steps(lax.broadcasted_iota(jnp.int32, (GRID, LANES), 0))
    damp = jnp.exp(-spread * (steps * steps))
    sine, cosine = sincos(flat[0:1] * steps)
    sine, cosine = sine * damp, cosine * damp
    power = jnp.where(lax.broadcasted_iota(jnp.int32, (GRID, LANES), 1) < HALF, 1.0, steps)
    gap = jnp.zeros((LANES - GRID, LANES), jnp.float32)
    for pair in range(2):
        c, s = power * cosine, power * sine
        for at, pieces in enumerate(((c, gap, s, gap), (s, gap, -c, gap))):
            high, low = split(jnp.concatenate(pieces, axis=0))
            cols = slice((2 * at + pair) * LANES, (2 * at + pair + 1) * LANES)
            left_ref[0, :, cols] = high
            left_ref[1, :, cols] = low
        power = power * (steps * steps)
    number = lax.broadcasted_iota(jnp.int32, (GRID, LANES), 0)
    line = signed_steps(FOLD * (number % (GRID // FOLD)) + number // (GRID // FOLD))
    damp = jnp.exp(-spread * (line * line))
    sine, cosine = sincos(flat[1:2] * line)
    siny_ref[...] = sine * damp
    cosy_ref[...] = cosine * damp
    planes = wave_ref.shape[0] * LANES // (2 * GRID * GRID)
    depth = sinz_ref.shape[0]
    deep = signed_steps(g * planes + lax.broadcasted_iota(jnp.int32, (depth, LANES), 0))
    sine, cosine = sincos(flat[2:3] * deep)
    damp = jnp.exp(-spread * (deep * deep))
    sinz_ref[...] = sine * damp
    cosz_ref[...] = cosine * damp

    band = lax.broadcasted_iota(jnp.int32, (LANES, bcount), 1) + b * bcount
    lane = lax.broadcasted_iota(jnp.int32, (SUB, LANES), 1)
    row = lax.broadcasted_iota(jnp.int32, (SUB, LANES), 0)
    shifts = [NPROJ * row + (at * LANES + lane) % NPROJ for at in range(PAD // LANES)]
    past = lax.broadcasted_iota(jnp.int32, (WIN, LANES), 1) - lax.broadcasted_iota(
        jnp.int32, (WIN, LANES), 0) // NPROJ * NPROJ

    def turn(n, xt_ref, t):
        s, group = n // groups, n % groups
        cols = slice(t*LANES, (t+1)*LANES)
        for k in range(kcount):
            mask = (band < occ_ref[s, k]).astype(jnp.float32).astype(jnp.bfloat16)
            for c in range(2):
                v = x_ref[s, group, c, k, :, cols].T * mask
                at = t*LANES
                while at < (t+1)*LANES:
                    w = at // WIN
                    end = min((w+1)*WIN, (t+1)*LANES)
                    xt_ref[k, w, (1 - c) * WIN + at - w*WIN:(1 - c) * WIN + end - w*WIN, :] = v[at - t*LANES:end - t*LANES]
                    at = end

    def window(n, xt_ref, w):
        s, group = n // groups, n % groups
        base = (w*WIN)//LANES*LANES
        o = w*WIN - base
        win = slice(base, base + 2*LANES)
        take = past < o + NPROJ - LANES
        re = im = None
        for k in range(kcount):
            both = mdot(xt_ref[k, w], x_ref[s, group, 1, k, :, win])
            r = mdot(xt_ref[k, w, WIN:], x_ref[s, group, 0, k, :, win]) + both[:WIN]
            m = both[WIN:]
            weight = weight_ref[k]
            r = jnp.where(take, r[:, LANES:], r[:, :LANES]) * weight
            m = jnp.where(take, m[:, LANES:], m[:, :LANES]) * weight
            re = r if re is None else re + r
            im = m if im is None else im + m
        sc_ref[w % SLOTS, 0] = re
        sc_ref[w % SLOTS, 1] = im

    def unfold(n, w):
        s, group = n // groups, n % groups
        o = w*WIN % LANES
        lifts = [(o + shift) & (LANES - 1) for shift in shifts]
        for c in range(2):
            tiles = [None]*(PAD//LANES)
            for i in range(NPROJ):
                piece = sc_ref[w % SLOTS, c, pl.ds(i, SUB, stride=NPROJ), :]
                for at in range(i*NPROJ // LANES, (i*NPROJ + NPROJ - 1) // LANES + 1):
                    part = jnp.take_along_axis(piece, lifts[at], axis=1, mode="promise_in_bounds")
                    tiles[at] = part if tiles[at] is None else jnp.where(lane >= i*NPROJ - at*LANES, part, tiles[at])
            for at, v in enumerate(tiles):
                here = pl.multiple_of(group * group_atoms + w * SUB, SUB)
                t_ref[c, pl.ds(here, SUB), at*LANES:(at+1)*LANES] = v

    def step(n, here, there):
        after = jnp.minimum(n + 1, total - 1)

        @pl.when(n + 1 < total)
        def _():
            fetch(n + 1).wait()

        for w in range(width // WIN):
            window(n, here, w)
            turn(after, there, w)
            if w == 0:
                turn(after, there, width // LANES - 1)
            unfold(n, w)

    entry = lax.broadcasted_iota(jnp.int32, (atoms, PAD), 1)
    keep = (entry // NPROJ <= entry % NPROJ) & (entry < ENTRIES)

    def pack(s):
        fold = fold_ref[...]
        high, low = split(jnp.where(entry < ENTRIES, t_ref[1], 0.0))
        packed = jnp.where(keep, t_ref[0], 0.0) + (mdot(high, fold) + mdot(low, fold))
        high, low = split(packed)
        routed = mdot(route_ref[...], high) + mdot(route_ref[...], low)
        for o in range(owners):
            rows_ref[s, o // ba, o % ba] = routed[o * per:(o + 1) * per]

    turns = [t // 2 + 1 if t % 2 == 0 else ka - 1 - t // 2 for t in range(ka - 1)][::-1]

    def swap(s, turn, step):
        peer = lax.rem(b + step, ba)
        return pltpu.make_async_remote_copy(
            src_ref=rows_ref.at[s, lax.rem(k + turn, ka), peer],
            dst_ref=first.at[s, step - 1, turn],
            send_sem=send1.at[s, step - 1, turn],
            recv_sem=recv1.at[s, step - 1, turn],
            device_id={"ba": peer},
            device_id_type=mesh_id,
        )

    def hop(s, turn):
        return pltpu.make_async_remote_copy(
            src_ref=held.at[s, turn - 1],
            dst_ref=second.at[s, turn - 1],
            send_sem=send2.at[s, turn - 1],
            recv_sem=recv2.at[s, turn - 1],
            device_id={"ka": lax.rem(k + turn, ka)},
            device_id_type=mesh_id,
        )

    def share(step):
        return pltpu.make_async_remote_copy(
            src_ref=sent,
            dst_ref=third.at[step - 1],
            send_sem=send3.at[step - 1],
            recv_sem=recv3.at[step - 1],
            device_id={"ga": lax.rem(g + step, ga)},
            device_id_type=mesh_id,
        )

    def start_swaps(s):
        for turn in turns + [0]:
            for step in range(1, ba):
                swap(s, turn, step).start()

    def chip_sum(s, turn):
        value = rows_ref[s, lax.rem(k + turn, ka), b]
        for step in range(1, ba):
            swap(s, turn, step).wait_recv()
            value = value + first[s, step - 1, turn]
        return value

    def start_hops(s):
        for turn in turns:
            held[s, turn - 1] = chip_sum(s, turn)
            hop(s, turn).start()

    fetch(0).wait()
    for t in range(width // LANES):
        turn(0, xa_ref, t)
    for s in range(spins):
        if groups % 2 == 0:
            @pl.loop(s * groups // 2, (s + 1) * groups // 2)
            def _(pair):
                step(2 * pair, xa_ref, xb_ref)
                if s:
                    @pl.when(pair == s * groups // 2)
                    def _():
                        start_hops(s - 1)
                step(2 * pair + 1, xb_ref, xa_ref)
        else:
            for n in range(s * groups, (s + 1) * groups):
                step(n, *((xa_ref, xb_ref) if n % 2 == 0 else (xb_ref, xa_ref)))
                if s and n == s * groups:
                    start_hops(s - 1)
        if s == 0:
            others[0].wait()
            pl.semaphore_wait(barrier, ka + ba + ga - 3)
        pack(s)
        start_swaps(s)
    others[1].wait()

    def plane(z, carry, along):
        sums = list(carry)
        cz, sz = cosz_ref[pl.ds(z, 1), :], sinz_ref[pl.ds(z, 1), :]
        cy, sy = cosy_ref[...], siny_ref[...]
        cosine = cz * cy - sz * sy
        sine = sz * cy + cz * sy
        index = g * planes + z
        height = grid_step * jnp.where(index >= GRID // 2, index - GRID, index).astype(jnp.float32)
        at = 0
        for pair in range(2):
            wave = along[:, pair * LANES:(pair + 1) * LANES] * cosine
            wave = wave - along[:, (2 + pair) * LANES:(3 + pair) * LANES] * sine
            for j in range(4 - 2 * pair):
                part = jnp.sum(wave.reshape(GRID // SUB, SUB, LANES), axis=0)
                for _ in range(4 - 2 * pair - j):
                    sums[at] = sums[at] + part
                    part = part * height
                    at += 1
                wave = wave * line
        return tuple(sums)

    lanes = lax.broadcasted_iota(jnp.int32, (GRID // FOLD, LANES), 1)

    def rows_of(z, c):
        start = z * (2 * GRID * GRID // LANES) + c
        one, two, three = (
            wave_ref[pl.ds(start + 2 * j, GRID // FOLD, stride=2 * (FOLD - 1)), :]
            for j in range(FOLD - 1)
        )
        return jnp.concatenate([
            one,
            pltpu.roll(jnp.where(lanes >= 96, one, two), 32, 1),
            pltpu.roll(jnp.where(lanes >= 64, two, three), 64, 1),
            pltpu.roll(three, 96, 1),
        ], axis=0)

    def body(chunk, carry):
        value = jnp.concatenate([
            jnp.concatenate([rows_of(chunk * CHUNK + turn, c) for turn in range(CHUNK)], axis=0)
            for c in (1, 0)
        ], axis=1)
        high, low = split(value)
        along = mdot(high, left_ref[0]) + mdot(low, left_ref[0]) + mdot(high, left_ref[1])
        for turn in range(CHUNK):
            carry = plane(chunk * CHUNK + turn, carry, along[turn * GRID:(turn + 1) * GRID])
        return carry

    sums = (jnp.zeros((SUB, LANES), jnp.float32),) * 13
    sums = lax.fori_loop(0, 1, body, sums)
    start_hops(spins - 1)
    sums = lax.fori_loop(1, planes // CHUNK, body, sums)
    found = {}
    at = 0
    for pair in range(2):
        for j in range(4 - 2 * pair):
            for l in range(4 - 2 * pair - j):
                value = jnp.sum(sums[at], axis=0, keepdims=True)
                at += 1
                found[2 * pair, j, l] = value
                if 2 * pair + 1 + j + l <= 3:
                    found[2 * pair + 1, j, l] = pltpu.roll(value, HALF, 1)
    pieces = [found[power] for power in POWERS]
    mono = jnp.concatenate(pieces + [jnp.zeros((ROWS - len(pieces), LANES), jnp.float32)], axis=0)
    sent[...] = mono
    for step in range(1, ga):
        share(step).start()
    others[2].wait()
    real = None
    for s in range(spins):
        value = chip_sum(s, 0)
        for turn in turns[::-1]:
            hop(s, turn).wait_recv()
            value = value + second[s, turn - 1]
        high, low = split(value)
        whole = mdot(high, open_ref[...]) + mdot(low, open_ref[...])
        density_ref[s, 0] = whole[:, :ENTRIES]
        density_ref[s, 1] = whole[:, PAD:PAD + ENTRIES]
        real = whole[:, :ENTRIES] if real is None else real + whole[:, :ENTRIES]
    moments = lax.dot_general(
        multipole_ref[...], real, (((1,), (1,)), ((), ())), precision=highest,
        preferred_element_type=jnp.float32,
    )
    for step in range(1, ga):
        share(step).wait_recv()
        mono = mono + third[step - 1]
    mono = jnp.where(lax.broadcasted_iota(jnp.int32, (ROWS, LANES), 0) == KIND_ROW, kinds, mono)
    mine = mono
    for block in range(1, blocks):
        mine = jnp.where(g == block, pltpu.roll(mono, LANES - block * per, 1), mine)
    mine = mine[:, :per]
    moments = jnp.where(mine[KIND_ROW:KIND_ROW + 1] == 0.0, moments[:NL], moments[NL:])
    for c in range(3):
        force = None
        for l, shape in enumerate(SHAPES):
            term = None
            for power, factor in shape.items():
                at = POWERS.index(tuple(p + (axis == c) for axis, p in enumerate(power)))
                part = mine[at:at + 1] * factor
                term = part if term is None else term + part
            term = term * moments[l:l + 1]
            force = term if force is None else force + term
        force_ref[c:c + 1, :] = force
    for s in range(spins):
        for turn in turns + [0]:
            for step in range(1, ba):
                swap(s, turn, step).wait_send()
        for turn in turns:
            hop(s, turn).wait_send()
    for step in range(1, ga):
        share(step).wait_send()


def shards(
    coefficients, occupied, kweights, owner_map, species, positions, multipole, widths, potential
):
    spins, parts, kcount, bcount, columns = coefficients.shape
    ka, ba, ga = (lax.axis_size(name) for name in ("ka", "ba", "ga"))
    width = group_width()
    groups = columns // width
    atoms = columns // NPROJ
    per = atoms // (ka * ba)
    planes = potential.shape[1] // (GRID * GRID)
    deep = -(-planes // SUB) * SUB
    wave = potential.reshape(2, -1, LANES).transpose(1, 0, 2).reshape(-1, LANES)
    vmem = pl.BlockSpec(memory_space=pltpu.VMEM)
    smem = pl.BlockSpec(memory_space=pltpu.SMEM)
    hbm = pl.BlockSpec(memory_space=pl.ANY)
    f32, bf16 = jnp.float32, jnp.bfloat16
    dma = pltpu.SemaphoreType.DMA
    return pl.pallas_call(
        main_kernel,
        out_shape=(
            jax.ShapeDtypeStruct((spins, parts, per, ENTRIES), f32),
            jax.ShapeDtypeStruct((3, per), f32),
        ),
        in_specs=[smem] * 3 + [hbm] * 4 + [vmem] * 4,
        out_specs=(vmem, vmem),
        scratch_shapes=[
            pltpu.VMEM((spins, groups, parts, kcount, bcount, width), bf16),
            *[pltpu.VMEM((kcount, width // WIN, 2 * WIN, bcount), bf16)] * 2,
            pltpu.VMEM((SLOTS, 2, WIN, LANES), f32),
            pltpu.VMEM((2, atoms, PAD), f32),
            pltpu.VMEM((atoms, atoms), bf16),
            pltpu.VMEM((spins, ka, ba, per, PAD), f32),
            pltpu.VMEM((spins, ba - 1, ka, per, PAD), f32),
            pltpu.VMEM((spins, ka - 1, per, PAD), f32),
            pltpu.VMEM((spins, ka - 1, per, PAD), f32),
            pltpu.VMEM((ROWS, LANES), f32),
            pltpu.VMEM((ga - 1, ROWS, LANES), f32),
            pltpu.VMEM(wave.shape, f32),
            pltpu.VMEM((PAD, PAD), bf16),
            pltpu.VMEM((PAD, 2 * PAD), bf16),
            pltpu.VMEM((2, 2 * LANES, 4 * LANES), bf16),
            pltpu.VMEM((GRID, LANES), f32),
            pltpu.VMEM((GRID, LANES), f32),
            pltpu.VMEM((deep, LANES), f32),
            pltpu.VMEM((deep, LANES), f32),
            dma((spins, groups)),
            dma((3,)),
            dma((spins, ba - 1, ka)),
            dma((spins, ba - 1, ka)),
            dma((spins, ka - 1)),
            dma((spins, ka - 1)),
            dma((ga - 1,)),
            dma((ga - 1,)),
        ],
        compiler_params=pltpu.CompilerParams(
            collective_id=0, has_side_effects=True, vmem_limit_bytes=63 * 2**20
        ),
    )(
        occupied, kweights, widths, coefficients, wave,
        jnp.asarray(fold_table(), bf16), jnp.asarray(open_table(), bf16),
        owner_map.reshape(1, -1), species.reshape(1, -1), positions,
        multipole.reshape(SPECIES * NL, ENTRIES),
    )


def solution(mesh):
    placed = (
        P(None, None, ("grp", "ka"), "ba", "ga"),
        P(None, ("grp", "ka")),
        P(("grp", "ka")),
        P("grp"),
        P("grp"),
        P(None, "grp"),
        P(),
        P(),
        P(None, ("grp", "ga")),
    )
    return jax.shard_map(
        shards,
        mesh=mesh,
        in_specs=placed,
        out_specs=(
            P(None, None, ("grp", "ka", "ga", "ba"), None),
            P(None, ("grp", "ka", "ga", "ba")),
        ),
        check_vma=False,
    )
```

```python
import functools
import math

import jax
import jax.numpy as jnp
import numpy as np
from jax import lax
from jax.experimental import pallas as pl
from jax.experimental.pallas import tpu as pltpu
from jax.sharding import PartitionSpec as P

NPROJ = 18
SPECIES = 2
NL = 9
GRID = 96
LANES = 128
SUB = 8
ENTRIES = NPROJ * NPROJ
PAD = -(-ENTRIES // LANES) * LANES
WIN = SUB * NPROJ
SLOTS = 2
HALF = LANES // 2
CHUNK = 3
FOLD = 4

grid_step = 0.0625
highest = lax.Precision.HIGHEST


def group_width():
    return NPROJ * LANES // math.gcd(NPROJ, LANES)


@functools.lru_cache(None)
def fold_table():
    q = np.zeros((PAD, PAD), np.float32)
    for i in range(NPROJ):
        for j in range(i):
            q[i * NPROJ + j, i * NPROJ + j] += 1.0
            q[j * NPROJ + i, i * NPROJ + j] -= 1.0
    return q


@functools.lru_cache(None)
def open_table():
    u = np.zeros((PAD, 2 * PAD), np.float32)
    for i in range(NPROJ):
        for j in range(NPROJ):
            u[min(i, j) * NPROJ + max(i, j), i * NPROJ + j] = 1.0
            if i > j:
                u[i * NPROJ + j, PAD + i * NPROJ + j] = 1.0
            elif i < j:
                u[j * NPROJ + i, PAD + i * NPROJ + j] = -1.0
    return u


POWERS = [(i, j, k) for i in range(4) for j in range(4 - i) for k in range(4 - i - j)]
SHAPES = [
    {(0, 0, 0): 1.0},
    {(1, 0, 0): 1.0},
    {(0, 1, 0): 1.0},
    {(0, 0, 1): 1.0},
    {(1, 1, 0): 1.0},
    {(0, 1, 1): 1.0},
    {(1, 0, 1): 1.0},
    {(2, 0, 0): 1.0, (0, 2, 0): -1.0},
    {(0, 0, 2): 2.0, (2, 0, 0): -1.0, (0, 2, 0): -1.0},
]
KIND_ROW = len(POWERS)
ROWS = -(-(KIND_ROW + 1) // SUB) * SUB


@functools.lru_cache(None)
def far_first(count):
    return [
        [(to - me) % count for to in sorted(range(count), key=lambda to: -abs(to - me)) if to != me]
        for me in range(count)
    ]


def split(value):
    high = value.astype(jnp.bfloat16)
    return high, (value - high.astype(jnp.float32)).astype(jnp.bfloat16)


def mdot(a, b):
    return jnp.dot(a, b, preferred_element_type=jnp.float32)


def flags(value):
    return value.astype(jnp.float32).astype(jnp.bfloat16)


def before(count):
    row = lax.broadcasted_iota(jnp.int32, (count, count), 0)
    col = lax.broadcasted_iota(jnp.int32, (count, count), 1)
    return flags(row < col)


def sincos(angle):
    turns = jnp.floor(angle * (2.0 / math.pi) + 0.5)
    rest = ((angle - turns * 1.5703125) - turns * 4.837512969970703125e-4) - turns * 7.54978995489188216e-8
    z = rest * rest
    sine = ((-1.9515295891e-4 * z + 8.3321608736e-3) * z - 1.6666654611e-1) * z * rest + rest
    cosine = (
        (2.443315711809948e-5 * z - 1.388731625493765e-3) * z + 4.166664568298827e-2
    ) * z * z - 0.5 * z + 1.0
    quarter = turns.astype(jnp.int32) & 3
    odd = (quarter & 1) == 1
    s = jnp.where(odd, cosine, sine)
    c = jnp.where(odd, sine, cosine)
    return jnp.where(quarter >= 2, -s, s), jnp.where((quarter == 1) | (quarter == 2), -c, c)


def signed_steps(index):
    return grid_step * jnp.where(index >= GRID // 2, index - GRID, index).astype(jnp.float32)


def main_kernel(
    x_hbm, occ_hbm, weight_hbm, width_hbm, owner_hbm, kind_hbm, place_hbm, multipole_hbm,
    wave_hbm, fold_hbm, open_hbm, density_hbm, force_hbm,
    occ_ref, weight_ref, width_ref, owner_ref, kind_ref, place_ref, multipole_ref,
    density_ref, force_ref, x_ref, xa_ref, xb_ref, sc_ref, t_ref, route_ref, rows_ref, first, held, second, sent, third,
    wave_ref, fold_ref, open_ref, left_ref, cosy_ref, siny_ref, cosz_ref, sinz_ref,
    sems, loads, stores, send1, recv1, send2, recv2, send3, recv3,
):
    mesh_id = pl.DeviceIdType.MESH
    ka, ba, ga = (lax.axis_size(name) for name in ("ka", "ba", "ga"))
    k, b, g = (lax.axis_index(name) for name in ("ka", "ba", "ga"))
    spins, groups, _, kcount, bcount, width = x_ref.shape
    atoms = t_ref.shape[1]
    per = rows_ref.shape[3]
    blocks = ga
    owners = ka * ba
    group_atoms = width // NPROJ
    total = spins * groups

    def fetch(n):
        s, group = n // groups, n % groups
        cols = pl.ds(pl.multiple_of(group * width, width), width)
        return pltpu.make_async_copy(
            x_hbm.at[s, :, :, :, cols], x_ref.at[s, group], sems.at[s, group]
        )

    others = [
        pltpu.make_async_copy(source, target, loads.at[at])
        for at, (source, target) in enumerate((
            (owner_hbm, owner_ref), (kind_hbm, kind_ref), (place_hbm, place_ref),
            (width_hbm, width_ref), (occ_hbm, occ_ref), (weight_hbm, weight_ref),
            (fold_hbm, fold_ref), (wave_hbm, wave_ref), (open_hbm, open_ref),
            (multipole_hbm, multipole_ref),
        ))
    ]
    for copy in others[:6]:
        copy.start()
    fetch(0).start()
    for n in range(1, total):
        fetch(n).start()
        if n == 1:
            for copy in others[6:]:
                copy.start()
    barrier = pltpu.get_barrier_semaphore()
    for name, me, size in (("ka", k, ka), ("ba", b, ba), ("ga", g, ga)):
        for step in range(1, size):
            pl.semaphore_signal(
                barrier, inc=1, device_id={name: lax.rem(me + step, size)}, device_id_type=mesh_id
            )

    for copy in others[:6]:
        copy.wait()
    owner = owner_ref[:, :atoms]
    for block in range(1, blocks):
        piece = owner_ref[:, block * atoms:(block + 1) * atoms]
        owner = jnp.where(g == block, piece, owner)
    lower = before(atoms)
    member = lax.broadcasted_iota(jnp.int32, (max(owners, 2 * SUB), atoms), 0) == owner
    count = mdot(flags(member), lower)
    rank = jnp.sum(jnp.where(member, count, 0.0), axis=0, keepdims=True)
    spot = owner.astype(jnp.float32) * per + rank
    place = lax.broadcasted_iota(jnp.int32, (atoms, atoms), 0).astype(jnp.float32)
    route_ref[...] = flags(place == spot)

    columns = []
    for block in range(blocks):
        span = slice(block * atoms, (block + 1) * atoms)
        mine = owner_ref[:, span] == k * ba + b
        rank = mdot(jnp.broadcast_to(flags(mine), (2 * SUB, atoms)), lower)[:1]
        spot = lax.broadcasted_iota(jnp.int32, (per, atoms), 0).astype(jnp.float32)
        chosen = mine & (rank == spot)
        columns.append([
            jnp.sum(jnp.where(chosen, value, 0.0), axis=1, keepdims=True)
            for value in (
                place_ref[0:1, span], place_ref[1:2, span], place_ref[2:3, span],
                kind_ref[:, span].astype(jnp.float32),
            )
        ])
    index = lax.broadcasted_iota(jnp.int32, (HALF, LANES), 1)
    table = jnp.zeros((HALF, LANES), jnp.float32)
    spare = HALF - blocks * per
    for at in range(4):
        pieces = [columns[block][at] for block in range(blocks)]
        if spare:
            pieces.append(jnp.zeros((spare, 1), jnp.float32))
        table = jnp.where(index == at, jnp.concatenate(pieces, axis=0), table)
    flat = jnp.concatenate([table, table], axis=0).T
    kinds = flat[3:4]
    spread = jnp.where(kinds == 0.0, width_ref[0], width_ref[1])

    steps = signed_steps(lax.broadcasted_iota(jnp.int32, (GRID, LANES), 0))
    damp = jnp.exp(-spread * (steps * steps))
    sine, cosine = sincos(flat[0:1] * steps)
    sine, cosine = sine * damp, cosine * damp
    power = jnp.where(lax.broadcasted_iota(jnp.int32, (GRID, LANES), 1) < HALF, 1.0, steps)
    gap = jnp.zeros((LANES - GRID, LANES), jnp.float32)
    for pair in range(2):
        c, s = power * cosine, power * sine
        for at, pieces in enumerate(((c, gap, s, gap), (s, gap, -c, gap))):
            high, low = split(jnp.concatenate(pieces, axis=0))
            cols = slice((2 * at + pair) * LANES, (2 * at + pair + 1) * LANES)
            left_ref[0, :, cols] = high
            left_ref[1, :, cols] = low
        power = power * (steps * steps)
    number = lax.broadcasted_iota(jnp.int32, (GRID, LANES), 0)
    line = signed_steps(FOLD * (number % (GRID // FOLD)) + number // (GRID // FOLD))
    damp = jnp.exp(-spread * (line * line))
    sine, cosine = sincos(flat[1:2] * line)
    siny_ref[...] = sine * damp
    cosy_ref[...] = cosine * damp
    planes = wave_ref.shape[0] * LANES // (2 * GRID * GRID)
    depth = sinz_ref.shape[0]
    deep = signed_steps(g * planes + lax.broadcasted_iota(jnp.int32, (depth, LANES), 0))
    sine, cosine = sincos(flat[2:3] * deep)
    damp = jnp.exp(-spread * (deep * deep))
    sinz_ref[...] = sine * damp
    cosz_ref[...] = cosine * damp

    band = lax.broadcasted_iota(jnp.int32, (LANES, bcount), 1) + b * bcount
    lane = lax.broadcasted_iota(jnp.int32, (SUB, LANES), 1)
    row = lax.broadcasted_iota(jnp.int32, (SUB, LANES), 0)
    shifts = [NPROJ * row + (at * LANES + lane) % NPROJ for at in range(PAD // LANES)]
    past = lax.broadcasted_iota(jnp.int32, (WIN, LANES), 1) - lax.broadcasted_iota(
        jnp.int32, (WIN, LANES), 0) // NPROJ * NPROJ

    def turn(n, xt_ref, t):
        s, group = n // groups, n % groups
        cols = slice(t*LANES, (t+1)*LANES)
        for k in range(kcount):
            mask = (band < occ_ref[s, k]).astype(jnp.float32).astype(jnp.bfloat16)
            for c in range(2):
                v = x_ref[s, group, c, k, :, cols].T * mask
                at = t*LANES
                while at < (t+1)*LANES:
                    w = at // WIN
                    end = min((w+1)*WIN, (t+1)*LANES)
                    xt_ref[k, w, (1 - c) * WIN + at - w*WIN:(1 - c) * WIN + end - w*WIN, :] = v[at - t*LANES:end - t*LANES]
                    at = end

    def window(n, xt_ref, w):
        s, group = n // groups, n % groups
        base = (w*WIN)//LANES*LANES
        o = w*WIN - base
        win = slice(base, base + 2*LANES)
        take = past < o + NPROJ - LANES
        re = im = None
        for k in range(kcount):
            both = mdot(xt_ref[k, w], x_ref[s, group, 1, k, :, win])
            r = mdot(xt_ref[k, w, WIN:], x_ref[s, group, 0, k, :, win]) + both[:WIN]
            m = both[WIN:]
            weight = weight_ref[k]
            r = jnp.where(take, r[:, LANES:], r[:, :LANES]) * weight
            m = jnp.where(take, m[:, LANES:], m[:, :LANES]) * weight
            re = r if re is None else re + r
            im = m if im is None else im + m
        sc_ref[w % SLOTS, 0] = re
        sc_ref[w % SLOTS, 1] = im

    def unfold(n, w):
        s, group = n // groups, n % groups
        o = w*WIN % LANES
        lifts = [(o + shift) & (LANES - 1) for shift in shifts]
        for c in range(2):
            tiles = [None]*(PAD//LANES)
            for i in range(NPROJ):
                piece = sc_ref[w % SLOTS, c, pl.ds(i, SUB, stride=NPROJ), :]
                for at in range(i*NPROJ // LANES, (i*NPROJ + NPROJ - 1) // LANES + 1):
                    part = jnp.take_along_axis(piece, lifts[at], axis=1, mode="promise_in_bounds")
                    tiles[at] = part if tiles[at] is None else jnp.where(lane >= i*NPROJ - at*LANES, part, tiles[at])
            for at, v in enumerate(tiles):
                here = pl.multiple_of(group * group_atoms + w * SUB, SUB)
                t_ref[c, pl.ds(here, SUB), at*LANES:(at+1)*LANES] = v

    def step(n, here, there):
        after = jnp.minimum(n + 1, total - 1)

        @pl.when(n + 1 < total)
        def _():
            fetch(n + 1).wait()

        for w in range(width // WIN):
            window(n, here, w)
            turn(after, there, w)
            if w == 0:
                turn(after, there, width // LANES - 1)
            unfold(n, w)

    entry = lax.broadcasted_iota(jnp.int32, (atoms, PAD), 1)
    keep = (entry // NPROJ <= entry % NPROJ) & (entry < ENTRIES)

    def pack(s):
        fold = fold_ref[...]
        high, low = split(jnp.where(entry < ENTRIES, t_ref[1], 0.0))
        packed = jnp.where(keep, t_ref[0], 0.0) + (mdot(high, fold) + mdot(low, fold))
        high, low = split(packed)
        routed = mdot(route_ref[...], high) + mdot(route_ref[...], low)
        for o in range(owners):
            rows_ref[s, o // ba, o % ba] = routed[o * per:(o + 1) * per]

    turns = list(range(1, ka))
    order = []
    for at in range(ka - 1):
        ahead = 0
        for me, ranks in enumerate(far_first(ka)):
            ahead = ahead + ranks[at] * ((ka - lax.rem(k - me + ka, ka)) // ka)
        order.append(ahead)

    def swap(s, turn, step):
        peer = lax.rem(b + step, ba)
        return pltpu.make_async_remote_copy(
            src_ref=rows_ref.at[s, lax.rem(k + turn, ka), peer],
            dst_ref=first.at[s, step - 1, turn],
            send_sem=send1.at[s, step - 1, turn],
            recv_sem=recv1.at[s, step - 1, turn],
            device_id={"ba": peer},
            device_id_type=mesh_id,
        )

    def hop(s, turn):
        return pltpu.make_async_remote_copy(
            src_ref=held.at[s, turn - 1],
            dst_ref=second.at[s, turn - 1],
            send_sem=send2.at[s, turn - 1],
            recv_sem=recv2.at[s, turn - 1],
            device_id={"ka": lax.rem(k + turn, ka)},
            device_id_type=mesh_id,
        )

    def share(step):
        return pltpu.make_async_remote_copy(
            src_ref=sent,
            dst_ref=third.at[step - 1],
            send_sem=send3.at[step - 1],
            recv_sem=recv3.at[step - 1],
            device_id={"ga": lax.rem(g + step, ga)},
            device_id_type=mesh_id,
        )

    def start_swaps(s):
        for turn in order + [0]:
            for step in range(1, ba):
                swap(s, turn, step).start()

    def chip_sum(s, turn):
        value = rows_ref[s, lax.rem(k + turn, ka), b]
        for step in range(1, ba):
            swap(s, turn, step).wait_recv()
            value = value + first[s, step - 1, turn]
        return value

    def start_hops(s):
        for turn in order:
            held[s, turn - 1] = chip_sum(s, turn)
            hop(s, turn).start()

    fetch(0).wait()
    for t in range(width // LANES):
        turn(0, xa_ref, t)
    for s in range(spins):
        if groups % 2 == 0:
            @pl.loop(s * groups // 2, (s + 1) * groups // 2)
            def _(pair):
                step(2 * pair, xa_ref, xb_ref)
                if s:
                    @pl.when(pair == s * groups // 2)
                    def _():
                        start_hops(s - 1)
                step(2 * pair + 1, xb_ref, xa_ref)
        else:
            for n in range(s * groups, (s + 1) * groups):
                step(n, *((xa_ref, xb_ref) if n % 2 == 0 else (xb_ref, xa_ref)))
                if s and n == s * groups:
                    start_hops(s - 1)
        if s == 0:
            others[6].wait()
            pl.semaphore_wait(barrier, ka + ba + ga - 3)
        pack(s)
        start_swaps(s)
    others[7].wait()

    def plane(z, carry, along):
        sums = list(carry)
        cz, sz = cosz_ref[pl.ds(z, 1), :], sinz_ref[pl.ds(z, 1), :]
        cy, sy = cosy_ref[...], siny_ref[...]
        cosine = cz * cy - sz * sy
        sine = sz * cy + cz * sy
        index = g * planes + z
        height = grid_step * jnp.where(index >= GRID // 2, index - GRID, index).astype(jnp.float32)
        at = 0
        for pair in range(2):
            wave = along[:, pair * LANES:(pair + 1) * LANES] * cosine
            wave = wave - along[:, (2 + pair) * LANES:(3 + pair) * LANES] * sine
            for j in range(4 - 2 * pair):
                part = jnp.sum(wave.reshape(GRID // SUB, SUB, LANES), axis=0)
                for _ in range(4 - 2 * pair - j):
                    sums[at] = sums[at] + part
                    part = part * height
                    at += 1
                wave = wave * line
        return tuple(sums)

    lanes = lax.broadcasted_iota(jnp.int32, (GRID // FOLD, LANES), 1)

    def rows_of(z, c):
        start = z * (2 * GRID * GRID // LANES) + c
        one, two, three = (
            wave_ref[pl.ds(start + 2 * j, GRID // FOLD, stride=2 * (FOLD - 1)), :]
            for j in range(FOLD - 1)
        )
        return jnp.concatenate([
            one,
            pltpu.roll(jnp.where(lanes >= 96, one, two), 32, 1),
            pltpu.roll(jnp.where(lanes >= 64, two, three), 64, 1),
            pltpu.roll(three, 96, 1),
        ], axis=0)

    def body(chunk, carry):
        value = jnp.concatenate([
            jnp.concatenate([rows_of(chunk * CHUNK + turn, c) for turn in range(CHUNK)], axis=0)
            for c in (1, 0)
        ], axis=1)
        high, low = split(value)
        along = mdot(high, left_ref[0]) + mdot(low, left_ref[0]) + mdot(high, left_ref[1])
        for turn in range(CHUNK):
            carry = plane(chunk * CHUNK + turn, carry, along[turn * GRID:(turn + 1) * GRID])
        return carry

    sums = (jnp.zeros((SUB, LANES), jnp.float32),) * 13
    sums = lax.fori_loop(0, 1, body, sums)
    start_hops(spins - 1)
    sums = lax.fori_loop(1, planes // CHUNK, body, sums)
    found = {}
    at = 0
    for pair in range(2):
        for j in range(4 - 2 * pair):
            for l in range(4 - 2 * pair - j):
                value = jnp.sum(sums[at], axis=0, keepdims=True)
                at += 1
                found[2 * pair, j, l] = value
                if 2 * pair + 1 + j + l <= 3:
                    found[2 * pair + 1, j, l] = pltpu.roll(value, HALF, 1)
    pieces = [found[power] for power in POWERS]
    mono = jnp.concatenate(pieces + [jnp.zeros((ROWS - len(pieces), LANES), jnp.float32)], axis=0)
    sent[...] = mono
    for step in range(1, ga):
        share(step).start()
    others[8].wait()
    others[9].wait()
    real = None
    for s in range(spins):
        value = chip_sum(s, 0)
        for turn in turns[::-1]:
            hop(s, turn).wait_recv()
            value = value + second[s, turn - 1]
        high, low = split(value)
        whole = mdot(high, open_ref[...]) + mdot(low, open_ref[...])
        density_ref[s, 0] = whole[:, :ENTRIES]
        density_ref[s, 1] = whole[:, PAD:PAD + ENTRIES]
        pltpu.make_async_copy(density_ref.at[s], density_hbm.at[s], stores.at[s]).start()
        real = whole[:, :ENTRIES] if real is None else real + whole[:, :ENTRIES]
    moments = [
        lax.dot_general(
            multipole_ref[:, kind, :], real, (((1,), (1,)), ((), ())), precision=highest,
            preferred_element_type=jnp.float32,
        )
        for kind in range(SPECIES)
    ]
    for step in range(1, ga):
        share(step).wait_recv()
        mono = mono + third[step - 1]
    mono = jnp.where(lax.broadcasted_iota(jnp.int32, (ROWS, LANES), 0) == KIND_ROW, kinds, mono)
    mine = mono
    for block in range(1, blocks):
        mine = jnp.where(g == block, pltpu.roll(mono, LANES - block * per, 1), mine)
    mine = mine[:, :per]
    moments = jnp.where(mine[KIND_ROW:KIND_ROW + 1] == 0.0, moments[0], moments[1])
    for c in range(3):
        force = None
        for l, shape in enumerate(SHAPES):
            term = None
            for power, factor in shape.items():
                at = POWERS.index(tuple(p + (axis == c) for axis, p in enumerate(power)))
                part = mine[at:at + 1] * factor
                term = part if term is None else term + part
            term = term * moments[l:l + 1]
            force = term if force is None else force + term
        force_ref[c:c + 1, :] = force
    stored = [
        pltpu.make_async_copy(density_ref.at[s], density_hbm.at[s], stores.at[s])
        for s in range(spins)
    ] + [pltpu.make_async_copy(force_ref, force_hbm, stores.at[spins])]
    stored[-1].start()
    for copy in stored:
        copy.wait()
    for s in range(spins):
        for turn in turns + [0]:
            for step in range(1, ba):
                swap(s, turn, step).wait_send()
        for turn in turns:
            hop(s, turn).wait_send()
    for step in range(1, ga):
        share(step).wait_send()


def settle_kernel(density_in, force_in, density_out, force_out, density, force, loads, stores):
    pairs = ((density_in, density, density_out), (force_in, force, force_out))
    into = [pltpu.make_async_copy(a, v, loads.at[at]) for at, (a, v, _) in enumerate(pairs)]
    away = [pltpu.make_async_copy(v, o, stores.at[at]) for at, (_, v, o) in enumerate(pairs)]
    for copy in into:
        copy.start()
    for first, second in zip(into, away):
        first.wait()
        second.start()
    for copy in away:
        copy.wait()


def shards(
    coefficients, occupied, kweights, owner_map, species, positions, multipole, widths, potential
):
    spins, parts, kcount, bcount, columns = coefficients.shape
    ka, ba, ga = (lax.axis_size(name) for name in ("ka", "ba", "ga"))
    width = group_width()
    groups = columns // width
    atoms = columns // NPROJ
    per = atoms // (ka * ba)
    planes = potential.shape[1] // (GRID * GRID)
    deep = -(-planes // SUB) * SUB
    wave = potential.reshape(2, -1, LANES).transpose(1, 0, 2).reshape(-1, LANES)
    hbm = pl.BlockSpec(memory_space=pl.ANY)
    f32, bf16 = jnp.float32, jnp.bfloat16
    dma = pltpu.SemaphoreType.DMA
    results = (
        jax.ShapeDtypeStruct((spins, parts, per, ENTRIES), f32),
        jax.ShapeDtypeStruct((3, per), f32),
    )
    outcome = pl.pallas_call(
        main_kernel,
        out_shape=results,
        in_specs=[hbm] * 11,
        out_specs=(hbm, hbm),
        scratch_shapes=[
            pltpu.SMEM(occupied.shape, jnp.int32),
            pltpu.SMEM(kweights.shape, f32),
            pltpu.SMEM(widths.shape, f32),
            pltpu.VMEM((1, *owner_map.shape), jnp.int32),
            pltpu.VMEM((1, *species.shape), jnp.int32),
            pltpu.VMEM(positions.shape, f32),
            pltpu.VMEM((NL, SPECIES, ENTRIES), f32),
            *[pltpu.VMEM(result.shape, f32) for result in results],
            pltpu.VMEM((spins, groups, parts, kcount, bcount, width), bf16),
            *[pltpu.VMEM((kcount, width // WIN, 2 * WIN, bcount), bf16)] * 2,
            pltpu.VMEM((SLOTS, 2, WIN, LANES), f32),
            pltpu.VMEM((2, atoms, PAD), f32),
            pltpu.VMEM((atoms, atoms), bf16),
            pltpu.VMEM((spins, ka, ba, per, PAD), f32),
            pltpu.VMEM((spins, ba - 1, ka, per, PAD), f32),
            pltpu.VMEM((spins, ka - 1, per, PAD), f32),
            pltpu.VMEM((spins, ka - 1, per, PAD), f32),
            pltpu.VMEM((ROWS, LANES), f32),
            pltpu.VMEM((ga - 1, ROWS, LANES), f32),
            pltpu.VMEM(wave.shape, f32),
            pltpu.VMEM((PAD, PAD), bf16),
            pltpu.VMEM((PAD, 2 * PAD), bf16),
            pltpu.VMEM((2, 2 * LANES, 4 * LANES), bf16),
            pltpu.VMEM((GRID, LANES), f32),
            pltpu.VMEM((GRID, LANES), f32),
            pltpu.VMEM((deep, LANES), f32),
            pltpu.VMEM((deep, LANES), f32),
            dma((spins, groups)),
            dma((10,)),
            dma((spins + 1,)),
            dma((spins, ba - 1, ka)),
            dma((spins, ba - 1, ka)),
            dma((spins, ka - 1)),
            dma((spins, ka - 1)),
            dma((ga - 1,)),
            dma((ga - 1,)),
        ],
        compiler_params=pltpu.CompilerParams(
            collective_id=0, has_side_effects=True, vmem_limit_bytes=63 * 2**20,
        ),
    )(
        coefficients, occupied, kweights, widths, owner_map.reshape(1, -1),
        species.reshape(1, -1), positions, multipole.transpose(1, 0, 2), wave,
        jnp.asarray(fold_table(), bf16), jnp.asarray(open_table(), bf16),
    )
    return pl.pallas_call(
        settle_kernel,
        out_shape=results,
        in_specs=[hbm, hbm],
        out_specs=(hbm, hbm),
        scratch_shapes=[*[pltpu.VMEM(result.shape, f32) for result in results], dma((2,)), dma((2,))],
    )(*outcome)


def solution(mesh):
    placed = (
        P(None, None, ("grp", "ka"), "ba", "ga"),
        P(None, ("grp", "ka")),
        P(("grp", "ka")),
        P("grp"),
        P("grp"),
        P(None, "grp"),
        P(),
        P(),
        P(None, ("grp", "ga")),
    )
    return jax.shard_map(
        shards,
        mesh=mesh,
        in_specs=placed,
        out_specs=(
            P(None, None, ("grp", "ka", "ga", "ba"), None),
            P(None, ("grp", "ka", "ga", "ba")),
        ),
        check_vma=False,
    )
```

```python
import functools
import math

import jax
import jax.numpy as jnp
import numpy as np
from jax import lax
from jax.experimental import pallas as pl
from jax.experimental.pallas import tpu as pltpu
from jax.sharding import PartitionSpec as P

NPROJ = 18
SPECIES = 2
NL = 9
GRID = 96
LANES = 128
SUB = 8
ENTRIES = NPROJ * NPROJ
PAD = -(-ENTRIES // LANES) * LANES
WIN = SUB * NPROJ
SLOTS = 2
HALF = LANES // 2
CHUNK = 3
FOLD = 4

grid_step = 0.0625
highest = lax.Precision.HIGHEST


def group_width():
    return NPROJ * LANES // math.gcd(NPROJ, LANES)


@functools.lru_cache(None)
def fold_table():
    q = np.zeros((PAD, PAD), np.float32)
    for i in range(NPROJ):
        for j in range(i):
            q[i * NPROJ + j, i * NPROJ + j] += 1.0
            q[j * NPROJ + i, i * NPROJ + j] -= 1.0
    return q


@functools.lru_cache(None)
def open_table():
    u = np.zeros((PAD, 2 * PAD), np.float32)
    for i in range(NPROJ):
        for j in range(NPROJ):
            u[min(i, j) * NPROJ + max(i, j), i * NPROJ + j] = 1.0
            if i > j:
                u[i * NPROJ + j, PAD + i * NPROJ + j] = 1.0
            elif i < j:
                u[j * NPROJ + i, PAD + i * NPROJ + j] = -1.0
    return u


POWERS = [(i, j, k) for i in range(4) for j in range(4 - i) for k in range(4 - i - j)]
SHAPES = [
    {(0, 0, 0): 1.0},
    {(1, 0, 0): 1.0},
    {(0, 1, 0): 1.0},
    {(0, 0, 1): 1.0},
    {(1, 1, 0): 1.0},
    {(0, 1, 1): 1.0},
    {(1, 0, 1): 1.0},
    {(2, 0, 0): 1.0, (0, 2, 0): -1.0},
    {(0, 0, 2): 2.0, (2, 0, 0): -1.0, (0, 2, 0): -1.0},
]
KIND_ROW = len(POWERS)
ROWS = -(-(KIND_ROW + 1) // SUB) * SUB


@functools.lru_cache(None)
def far_first(count):
    return [
        [(to - me) % count for to in sorted(range(count), key=lambda to: -abs(to - me)) if to != me]
        for me in range(count)
    ]


def split(value):
    high = value.astype(jnp.bfloat16)
    return high, (value - high.astype(jnp.float32)).astype(jnp.bfloat16)


def mdot(a, b):
    return jnp.dot(a, b, preferred_element_type=jnp.float32)


def flags(value):
    return value.astype(jnp.float32).astype(jnp.bfloat16)


def before(count):
    row = lax.broadcasted_iota(jnp.int32, (count, count), 0)
    col = lax.broadcasted_iota(jnp.int32, (count, count), 1)
    return flags(row < col)


def sincos(angle):
    turns = jnp.floor(angle * (2.0 / math.pi) + 0.5)
    rest = ((angle - turns * 1.5703125) - turns * 4.837512969970703125e-4) - turns * 7.54978995489188216e-8
    z = rest * rest
    sine = ((-1.9515295891e-4 * z + 8.3321608736e-3) * z - 1.6666654611e-1) * z * rest + rest
    cosine = (
        (2.443315711809948e-5 * z - 1.388731625493765e-3) * z + 4.166664568298827e-2
    ) * z * z - 0.5 * z + 1.0
    quarter = turns.astype(jnp.int32) & 3
    odd = (quarter & 1) == 1
    s = jnp.where(odd, cosine, sine)
    c = jnp.where(odd, sine, cosine)
    return jnp.where(quarter >= 2, -s, s), jnp.where((quarter == 1) | (quarter == 2), -c, c)


def signed_steps(index):
    return grid_step * jnp.where(index >= GRID // 2, index - GRID, index).astype(jnp.float32)


def main_kernel(
    x_hbm, occ_hbm, weight_hbm, width_hbm, owner_hbm, kind_hbm, place_hbm, multipole_hbm,
    wave_hbm, fold_hbm, open_hbm, density_hbm, force_hbm,
    occ_ref, weight_ref, width_ref, owner_ref, kind_ref, place_ref, multipole_ref,
    density_ref, force_ref, x_ref, xa_ref, xb_ref, sc_ref, t_ref, route_ref, rows_ref, first, held, second, sent, third,
    wave_ref, fold_ref, open_ref, left_ref, cosy_ref, siny_ref, cosz_ref, sinz_ref,
    sems, loads, stores, send1, recv1, send2, recv2, send3, recv3,
):
    mesh_id = pl.DeviceIdType.MESH
    ka, ba, ga = (lax.axis_size(name) for name in ("ka", "ba", "ga"))
    k, b, g = (lax.axis_index(name) for name in ("ka", "ba", "ga"))
    spins, groups, _, kcount, bcount, width = x_ref.shape
    atoms = t_ref.shape[1]
    per = rows_ref.shape[3]
    blocks = ga
    owners = ka * ba
    group_atoms = width // NPROJ
    total = spins * groups

    def fetch(n):
        s, group = n // groups, n % groups
        cols = pl.ds(pl.multiple_of(group * width, width), width)
        return pltpu.make_async_copy(
            x_hbm.at[s, :, :, :, cols], x_ref.at[s, group], sems.at[s, group]
        )

    others = [
        pltpu.make_async_copy(source, target, loads.at[at])
        for at, (source, target) in enumerate((
            (owner_hbm, owner_ref), (kind_hbm, kind_ref), (place_hbm, place_ref),
            (width_hbm, width_ref), (occ_hbm, occ_ref), (weight_hbm, weight_ref),
            (fold_hbm, fold_ref), (wave_hbm, wave_ref), (open_hbm, open_ref),
            (multipole_hbm, multipole_ref),
        ))
    ]
    for copy in others[:6]:
        copy.start()
    fetch(0).start()
    for n in range(1, total):
        fetch(n).start()
        if n == 1:
            for copy in others[6:]:
                copy.start()
    barrier = pltpu.get_barrier_semaphore()
    for name, me, size in (("ka", k, ka), ("ba", b, ba), ("ga", g, ga)):
        for step in range(1, size):
            pl.semaphore_signal(
                barrier, inc=1, device_id={name: lax.rem(me + step, size)}, device_id_type=mesh_id
            )

    for copy in others[:6]:
        copy.wait()
    owner = owner_ref[:, :atoms]
    for block in range(1, blocks):
        piece = owner_ref[:, block * atoms:(block + 1) * atoms]
        owner = jnp.where(g == block, piece, owner)
    lower = before(atoms)
    member = lax.broadcasted_iota(jnp.int32, (max(owners, 2 * SUB), atoms), 0) == owner
    count = mdot(flags(member), lower)
    rank = jnp.sum(jnp.where(member, count, 0.0), axis=0, keepdims=True)
    spot = owner.astype(jnp.float32) * per + rank
    place = lax.broadcasted_iota(jnp.int32, (atoms, atoms), 0).astype(jnp.float32)
    route_ref[...] = flags(place == spot)

    columns = []
    for block in range(blocks):
        span = slice(block * atoms, (block + 1) * atoms)
        mine = owner_ref[:, span] == k * ba + b
        rank = mdot(jnp.broadcast_to(flags(mine), (2 * SUB, atoms)), lower)[:1]
        spot = lax.broadcasted_iota(jnp.int32, (per, atoms), 0).astype(jnp.float32)
        chosen = mine & (rank == spot)
        columns.append([
            jnp.sum(jnp.where(chosen, value, 0.0), axis=1, keepdims=True)
            for value in (
                place_ref[0:1, span], place_ref[1:2, span], place_ref[2:3, span],
                kind_ref[:, span].astype(jnp.float32),
            )
        ])
    index = lax.broadcasted_iota(jnp.int32, (HALF, LANES), 1)
    table = jnp.zeros((HALF, LANES), jnp.float32)
    spare = HALF - blocks * per
    for at in range(4):
        pieces = [columns[block][at] for block in range(blocks)]
        if spare:
            pieces.append(jnp.zeros((spare, 1), jnp.float32))
        table = jnp.where(index == at, jnp.concatenate(pieces, axis=0), table)
    flat = jnp.concatenate([table, table], axis=0).T
    kinds = flat[3:4]
    spread = jnp.where(kinds == 0.0, width_ref[0], width_ref[1])

    steps = signed_steps(lax.broadcasted_iota(jnp.int32, (GRID, LANES), 0))
    damp = jnp.exp(-spread * (steps * steps))
    sine, cosine = sincos(flat[0:1] * steps)
    sine, cosine = sine * damp, cosine * damp
    power = jnp.where(lax.broadcasted_iota(jnp.int32, (GRID, LANES), 1) < HALF, 1.0, steps)
    gap = jnp.zeros((LANES - GRID, LANES), jnp.float32)
    for pair in range(2):
        c, s = power * cosine, power * sine
        for at, pieces in enumerate(((c, gap, s, gap), (s, gap, -c, gap))):
            high, low = split(jnp.concatenate(pieces, axis=0))
            cols = slice((2 * at + pair) * LANES, (2 * at + pair + 1) * LANES)
            left_ref[0, :, cols] = high
            left_ref[1, :, cols] = low
        power = power * (steps * steps)
    number = lax.broadcasted_iota(jnp.int32, (GRID, LANES), 0)
    line = signed_steps(FOLD * (number % (GRID // FOLD)) + number // (GRID // FOLD))
    damp = jnp.exp(-spread * (line * line))
    sine, cosine = sincos(flat[1:2] * line)
    siny_ref[...] = sine * damp
    cosy_ref[...] = cosine * damp
    planes = wave_ref.shape[0] * LANES // (2 * GRID * GRID)
    depth = sinz_ref.shape[0]
    deep = signed_steps(g * planes + lax.broadcasted_iota(jnp.int32, (depth, LANES), 0))
    sine, cosine = sincos(flat[2:3] * deep)
    damp = jnp.exp(-spread * (deep * deep))
    sinz_ref[...] = sine * damp
    cosz_ref[...] = cosine * damp

    band = lax.broadcasted_iota(jnp.int32, (LANES, bcount), 1) + b * bcount
    lane = lax.broadcasted_iota(jnp.int32, (SUB, LANES), 1)
    row = lax.broadcasted_iota(jnp.int32, (SUB, LANES), 0)
    shifts = [NPROJ * row + (at * LANES + lane) % NPROJ for at in range(PAD // LANES)]
    past = lax.broadcasted_iota(jnp.int32, (WIN, LANES), 1) - lax.broadcasted_iota(
        jnp.int32, (WIN, LANES), 0) // NPROJ * NPROJ

    def turn(n, xt_ref, t):
        s, group = n // groups, n % groups
        cols = slice(t*LANES, (t+1)*LANES)
        for k in range(kcount):
            mask = (band < occ_ref[s, k]).astype(jnp.float32).astype(jnp.bfloat16)
            for c in range(2):
                v = x_ref[s, group, c, k, :, cols].T * mask
                at = t*LANES
                while at < (t+1)*LANES:
                    w = at // WIN
                    end = min((w+1)*WIN, (t+1)*LANES)
                    xt_ref[k, w, (1 - c) * WIN + at - w*WIN:(1 - c) * WIN + end - w*WIN, :] = v[at - t*LANES:end - t*LANES]
                    at = end

    def window(n, xt_ref, w):
        s, group = n // groups, n % groups
        base = (w*WIN)//LANES*LANES
        o = w*WIN - base
        win = slice(base, base + 2*LANES)
        take = past < o + NPROJ - LANES
        re = im = None
        for k in range(kcount):
            both = mdot(xt_ref[k, w], x_ref[s, group, 1, k, :, win])
            r = mdot(xt_ref[k, w, WIN:], x_ref[s, group, 0, k, :, win]) + both[:WIN]
            m = both[WIN:]
            weight = weight_ref[k]
            r = jnp.where(take, r[:, LANES:], r[:, :LANES]) * weight
            m = jnp.where(take, m[:, LANES:], m[:, :LANES]) * weight
            re = r if re is None else re + r
            im = m if im is None else im + m
        sc_ref[w % SLOTS, 0] = re
        sc_ref[w % SLOTS, 1] = im

    def unfold(n, w):
        s, group = n // groups, n % groups
        o = w*WIN % LANES
        lifts = [(o + shift) & (LANES - 1) for shift in shifts]
        for c in range(2):
            tiles = [None]*(PAD//LANES)
            for i in range(NPROJ):
                piece = sc_ref[w % SLOTS, c, pl.ds(i, SUB, stride=NPROJ), :]
                for at in range(i*NPROJ // LANES, (i*NPROJ + NPROJ - 1) // LANES + 1):
                    part = jnp.take_along_axis(piece, lifts[at], axis=1, mode="promise_in_bounds")
                    tiles[at] = part if tiles[at] is None else jnp.where(lane >= i*NPROJ - at*LANES, part, tiles[at])
            for at, v in enumerate(tiles):
                here = pl.multiple_of(group * group_atoms + w * SUB, SUB)
                t_ref[c, pl.ds(here, SUB), at*LANES:(at+1)*LANES] = v

    def step(n, here, there):
        after = jnp.minimum(n + 1, total - 1)

        @pl.when(n + 1 < total)
        def _():
            fetch(n + 1).wait()

        for w in range(width // WIN):
            window(n, here, w)
            turn(after, there, w)
            if w == 0:
                turn(after, there, width // LANES - 1)
            unfold(n, w)

    entry = lax.broadcasted_iota(jnp.int32, (atoms, PAD), 1)
    keep = (entry // NPROJ <= entry % NPROJ) & (entry < ENTRIES)

    def pack(s):
        fold = fold_ref[...]
        high, low = split(jnp.where(entry < ENTRIES, t_ref[1], 0.0))
        packed = jnp.where(keep, t_ref[0], 0.0) + mdot(
            jnp.concatenate([high, low], axis=1), jnp.concatenate([fold, fold], axis=0)
        )
        high, low = split(packed)
        routed = mdot(route_ref[...], high) + mdot(route_ref[...], low)
        for o in range(owners):
            rows_ref[s, o // ba, o % ba] = routed[o * per:(o + 1) * per]

    turns = list(range(1, ka))
    order = []
    for at in range(ka - 1):
        ahead = 0
        for me, ranks in enumerate(far_first(ka)):
            ahead = ahead + ranks[at] * ((ka - lax.rem(k - me + ka, ka)) // ka)
        order.append(ahead)

    def swap(s, turn, step):
        peer = lax.rem(b + step, ba)
        return pltpu.make_async_remote_copy(
            src_ref=rows_ref.at[s, lax.rem(k + turn, ka), peer],
            dst_ref=first.at[s, step - 1, turn],
            send_sem=send1.at[s, step - 1, turn],
            recv_sem=recv1.at[s, step - 1, turn],
            device_id={"ba": peer},
            device_id_type=mesh_id,
        )

    def hop(s, turn):
        return pltpu.make_async_remote_copy(
            src_ref=held.at[s, turn - 1],
            dst_ref=second.at[s, turn - 1],
            send_sem=send2.at[s, turn - 1],
            recv_sem=recv2.at[s, turn - 1],
            device_id={"ka": lax.rem(k + turn, ka)},
            device_id_type=mesh_id,
        )

    def share(step):
        return pltpu.make_async_remote_copy(
            src_ref=sent,
            dst_ref=third.at[step - 1],
            send_sem=send3.at[step - 1],
            recv_sem=recv3.at[step - 1],
            device_id={"ga": lax.rem(g + step, ga)},
            device_id_type=mesh_id,
        )

    def start_swaps(s):
        for turn in order + [0]:
            for step in range(1, ba):
                swap(s, turn, step).start()

    def chip_sum(s, turn):
        value = rows_ref[s, lax.rem(k + turn, ka), b]
        for step in range(1, ba):
            swap(s, turn, step).wait_recv()
            value = value + first[s, step - 1, turn]
        return value

    def start_hops(s):
        for turn in order:
            held[s, turn - 1] = chip_sum(s, turn)
            hop(s, turn).start()

    fetch(0).wait()
    for t in range(width // LANES):
        turn(0, xa_ref, t)
    for s in range(spins):
        if groups % 2 == 0:
            @pl.loop(s * groups // 2, (s + 1) * groups // 2)
            def _(pair):
                step(2 * pair, xa_ref, xb_ref)
                if s:
                    @pl.when(pair == s * groups // 2)
                    def _():
                        start_hops(s - 1)
                step(2 * pair + 1, xb_ref, xa_ref)
        else:
            for n in range(s * groups, (s + 1) * groups):
                step(n, *((xa_ref, xb_ref) if n % 2 == 0 else (xb_ref, xa_ref)))
                if s and n == s * groups:
                    start_hops(s - 1)
        if s == 0:
            others[6].wait()
            pl.semaphore_wait(barrier, ka + ba + ga - 3)
        pack(s)
        start_swaps(s)
    others[7].wait()

    def plane(z, carry, along):
        sums = list(carry)
        cz, sz = cosz_ref[pl.ds(z, 1), :], sinz_ref[pl.ds(z, 1), :]
        cy, sy = cosy_ref[...], siny_ref[...]
        cosine = cz * cy - sz * sy
        sine = sz * cy + cz * sy
        index = g * planes + z
        height = grid_step * jnp.where(index >= GRID // 2, index - GRID, index).astype(jnp.float32)
        at = 0
        for pair in range(2):
            wave = along[:, pair * LANES:(pair + 1) * LANES] * cosine
            wave = wave - along[:, (2 + pair) * LANES:(3 + pair) * LANES] * sine
            for j in range(4 - 2 * pair):
                part = jnp.sum(wave.reshape(GRID // SUB, SUB, LANES), axis=0)
                for _ in range(4 - 2 * pair - j):
                    sums[at] = sums[at] + part
                    part = part * height
                    at += 1
                wave = wave * line
        return tuple(sums)

    lanes = lax.broadcasted_iota(jnp.int32, (GRID // FOLD, LANES), 1)

    def rows_of(z, c):
        start = z * (2 * GRID * GRID // LANES) + c
        one, two, three = (
            wave_ref[pl.ds(start + 2 * j, GRID // FOLD, stride=2 * (FOLD - 1)), :]
            for j in range(FOLD - 1)
        )
        return jnp.concatenate([
            one,
            pltpu.roll(jnp.where(lanes >= 96, one, two), 32, 1),
            pltpu.roll(jnp.where(lanes >= 64, two, three), 64, 1),
            pltpu.roll(three, 96, 1),
        ], axis=0)

    def body(chunk, carry):
        value = jnp.concatenate([
            jnp.concatenate([rows_of(chunk * CHUNK + turn, c) for turn in range(CHUNK)], axis=0)
            for c in (1, 0)
        ], axis=1)
        high, low = split(value)
        along = mdot(high, left_ref[0]) + mdot(low, left_ref[0]) + mdot(high, left_ref[1])
        for turn in range(CHUNK):
            carry = plane(chunk * CHUNK + turn, carry, along[turn * GRID:(turn + 1) * GRID])
        return carry

    sums = (jnp.zeros((SUB, LANES), jnp.float32),) * 13
    sums = lax.fori_loop(0, 1, body, sums)
    start_hops(spins - 1)
    sums = lax.fori_loop(1, planes // CHUNK, body, sums)
    found = {}
    at = 0
    for pair in range(2):
        for j in range(4 - 2 * pair):
            for l in range(4 - 2 * pair - j):
                value = jnp.sum(sums[at], axis=0, keepdims=True)
                at += 1
                found[2 * pair, j, l] = value
                if 2 * pair + 1 + j + l <= 3:
                    found[2 * pair + 1, j, l] = pltpu.roll(value, HALF, 1)
    pieces = [found[power] for power in POWERS]
    mono = jnp.concatenate(pieces + [jnp.zeros((ROWS - len(pieces), LANES), jnp.float32)], axis=0)
    sent[...] = mono
    for step in range(1, ga):
        share(step).start()
    others[8].wait()
    others[9].wait()
    real = None
    for s in range(spins):
        value = chip_sum(s, 0)
        for turn in turns[::-1]:
            hop(s, turn).wait_recv()
            value = value + second[s, turn - 1]
        high, low = split(value)
        whole = mdot(high, open_ref[...]) + mdot(low, open_ref[...])
        density_ref[s, 0] = whole[:, :ENTRIES]
        density_ref[s, 1] = whole[:, PAD:PAD + ENTRIES]
        pltpu.make_async_copy(density_ref.at[s], density_hbm.at[s], stores.at[s]).start()
        real = whole[:, :ENTRIES] if real is None else real + whole[:, :ENTRIES]
    moments = [
        lax.dot_general(
            multipole_ref[:, kind, :], real, (((1,), (1,)), ((), ())), precision=highest,
            preferred_element_type=jnp.float32,
        )
        for kind in range(SPECIES)
    ]
    for step in range(1, ga):
        share(step).wait_recv()
        mono = mono + third[step - 1]
    mono = jnp.where(lax.broadcasted_iota(jnp.int32, (ROWS, LANES), 0) == KIND_ROW, kinds, mono)
    mine = mono
    for block in range(1, blocks):
        mine = jnp.where(g == block, pltpu.roll(mono, LANES - block * per, 1), mine)
    mine = mine[:, :per]
    moments = jnp.where(mine[KIND_ROW:KIND_ROW + 1] == 0.0, moments[0], moments[1])
    for c in range(3):
        force = None
        for l, shape in enumerate(SHAPES):
            term = None
            for power, factor in shape.items():
                at = POWERS.index(tuple(p + (axis == c) for axis, p in enumerate(power)))
                part = mine[at:at + 1] * factor
                term = part if term is None else term + part
            term = term * moments[l:l + 1]
            force = term if force is None else force + term
        force_ref[c:c + 1, :] = force
    stored = [
        pltpu.make_async_copy(density_ref.at[s], density_hbm.at[s], stores.at[s])
        for s in range(spins)
    ] + [pltpu.make_async_copy(force_ref, force_hbm, stores.at[spins])]
    stored[-1].start()
    for copy in stored:
        copy.wait()
    for s in range(spins):
        for turn in turns + [0]:
            for step in range(1, ba):
                swap(s, turn, step).wait_send()
        for turn in turns:
            hop(s, turn).wait_send()
    for step in range(1, ga):
        share(step).wait_send()


def settle_kernel(density_in, force_in, density_out, force_out, density, force, loads, stores):
    pairs = ((density_in, density, density_out), (force_in, force, force_out))
    into = [pltpu.make_async_copy(a, v, loads.at[at]) for at, (a, v, _) in enumerate(pairs)]
    away = [pltpu.make_async_copy(v, o, stores.at[at]) for at, (_, v, o) in enumerate(pairs)]
    for copy in into:
        copy.start()
    for first, second in zip(into, away):
        first.wait()
        second.start()
    for copy in away:
        copy.wait()


def shards(
    coefficients, occupied, kweights, owner_map, species, positions, multipole, widths, potential
):
    spins, parts, kcount, bcount, columns = coefficients.shape
    ka, ba, ga = (lax.axis_size(name) for name in ("ka", "ba", "ga"))
    width = group_width()
    groups = columns // width
    atoms = columns // NPROJ
    per = atoms // (ka * ba)
    planes = potential.shape[1] // (GRID * GRID)
    deep = -(-planes // SUB) * SUB
    wave = potential.reshape(2, -1, LANES).transpose(1, 0, 2).reshape(-1, LANES)
    hbm = pl.BlockSpec(memory_space=pl.ANY)
    f32, bf16 = jnp.float32, jnp.bfloat16
    dma = pltpu.SemaphoreType.DMA
    results = (
        jax.ShapeDtypeStruct((spins, parts, per, ENTRIES), f32),
        jax.ShapeDtypeStruct((3, per), f32),
    )
    outcome = pl.pallas_call(
        main_kernel,
        out_shape=results,
        in_specs=[hbm] * 11,
        out_specs=(hbm, hbm),
        scratch_shapes=[
            pltpu.SMEM(occupied.shape, jnp.int32),
            pltpu.SMEM(kweights.shape, f32),
            pltpu.SMEM(widths.shape, f32),
            pltpu.VMEM((1, *owner_map.shape), jnp.int32),
            pltpu.VMEM((1, *species.shape), jnp.int32),
            pltpu.VMEM(positions.shape, f32),
            pltpu.VMEM((NL, SPECIES, ENTRIES), f32),
            *[pltpu.VMEM(result.shape, f32) for result in results],
            pltpu.VMEM((spins, groups, parts, kcount, bcount, width), bf16),
            *[pltpu.VMEM((kcount, width // WIN, 2 * WIN, bcount), bf16)] * 2,
            pltpu.VMEM((SLOTS, 2, WIN, LANES), f32),
            pltpu.VMEM((2, atoms, PAD), f32),
            pltpu.VMEM((atoms, atoms), bf16),
            pltpu.VMEM((spins, ka, ba, per, PAD), f32),
            pltpu.VMEM((spins, ba - 1, ka, per, PAD), f32),
            pltpu.VMEM((spins, ka - 1, per, PAD), f32),
            pltpu.VMEM((spins, ka - 1, per, PAD), f32),
            pltpu.VMEM((ROWS, LANES), f32),
            pltpu.VMEM((ga - 1, ROWS, LANES), f32),
            pltpu.VMEM(wave.shape, f32),
            pltpu.VMEM((PAD, PAD), bf16),
            pltpu.VMEM((PAD, 2 * PAD), bf16),
            pltpu.VMEM((2, 2 * LANES, 4 * LANES), bf16),
            pltpu.VMEM((GRID, LANES), f32),
            pltpu.VMEM((GRID, LANES), f32),
            pltpu.VMEM((deep, LANES), f32),
            pltpu.VMEM((deep, LANES), f32),
            dma((spins, groups)),
            dma((10,)),
            dma((spins + 1,)),
            dma((spins, ba - 1, ka)),
            dma((spins, ba - 1, ka)),
            dma((spins, ka - 1)),
            dma((spins, ka - 1)),
            dma((ga - 1,)),
            dma((ga - 1,)),
        ],
        compiler_params=pltpu.CompilerParams(
            collective_id=0, has_side_effects=True, vmem_limit_bytes=63 * 2**20,
        ),
    )(
        coefficients, occupied, kweights, widths, owner_map.reshape(1, -1),
        species.reshape(1, -1), positions, multipole.transpose(1, 0, 2), wave,
        jnp.asarray(fold_table(), bf16), jnp.asarray(open_table(), bf16),
    )
    return pl.pallas_call(
        settle_kernel,
        out_shape=results,
        in_specs=[hbm, hbm],
        out_specs=(hbm, hbm),
        scratch_shapes=[*[pltpu.VMEM(result.shape, f32) for result in results], dma((2,)), dma((2,))],
    )(*outcome)


def solution(mesh):
    placed = (
        P(None, None, ("grp", "ka"), "ba", "ga"),
        P(None, ("grp", "ka")),
        P(("grp", "ka")),
        P("grp"),
        P("grp"),
        P(None, "grp"),
        P(),
        P(),
        P(None, ("grp", "ga")),
    )
    return jax.shard_map(
        shards,
        mesh=mesh,
        in_specs=placed,
        out_specs=(
            P(None, None, ("grp", "ka", "ga", "ba"), None),
            P(None, ("grp", "ka", "ga", "ba")),
        ),
        check_vma=False,
    )
```
